512 devices in a mesh: corpus: 256 (over y, z, x), dim: 2 (over core).
Axes of the slice: x: 4, y: 8, z: 8, core: 2. Of those that a mesh axis runs over, the one named last changes fastest.
Arguments:
- queries: bfloat16 [128, 768], P('dim'), as said below
- corpus: bfloat16 [131072, 768], P('corpus', 'dim'), as said below
- candidates: int32 [128, 1024], P('dim'), may hold values from 0 to 131071
Outputs:
- log_probs: float32 [128, 1024], P('dim', 'corpus')
The draws below stay inside these ranges and needn't reach their ends.
Inputs may be any that keep to these rules, and one draw needn't show every extreme that they name: `queries`: query rows have real entries of moderate size; their norms differ from row to row. `corpus`: corpus rows have real entries of moderate size; their norms differ from row to row.
All inputs are finite; a program needn't handle non-finite values.
Results may differ from the reference program's by a relative error of at most 0.00095.
Values may be sent and summed in bfloat16 or wider, within the bound.
No kernel may reach another device: no remote copies, remote signals or barrier semaphores. Data moves between devices by JAX's collectives and lax.ppermute only.
A program may use at most 64 MiB of HBM per device.

```python
import math
import jax
import jax.numpy as jnp
from jax import lax

D = 768
Q = 128
ROWS_DEV = 512
K = 1024
CORPUS = 131072
N_CORPUS = 256


def corpus_row(key, index):
    base = jax.random.fold_in(key, 11)
    own = jax.random.fold_in(base, index)
    gauss = jax.random.normal(jax.random.fold_in(own, 3), (D,), jnp.float32)
    scale = jnp.exp(jax.random.uniform(jax.random.fold_in(own, 4), (), jnp.float32, math.log(0.5), math.log(1.5)))
    return gauss * scale * 3.0 / math.sqrt(D)


def draw_corpus(key, part):
    indices = jnp.arange(CORPUS, dtype=jnp.int32)
    rows = jax.vmap(lambda index: corpus_row(key, index))(indices)
    return rows.astype(jnp.bfloat16)


def draw_queries(key, part):
    own = jax.random.fold_in(key, 23)
    scales = jnp.exp(jax.random.uniform(jax.random.fold_in(own, 1), (Q, 1), jnp.float32, math.log(0.3), math.log(3.0)))
    drawn = jax.random.normal(jax.random.fold_in(own, 2), (Q, D), jnp.float32) * scales
    return drawn.astype(jnp.bfloat16)


def set_ends(values, stream_key, smallest, largest):
    index_at = [jax.random.randint(jax.random.fold_in(stream_key, axis), (), 0, length) for axis, length in enumerate(values.shape)]
    widest = values.shape.index(max(values.shape))
    neighbour = index_at[:widest] + [(index_at[widest] + 1) % values.shape[widest]] + index_at[widest + 1:]
    return values.at[tuple(index_at)].set(smallest).at[tuple(neighbour)].set(largest)


def setup_inputs(seed: int = 0) -> dict:
    arg_keys = jax.random.split(jax.random.key(seed), 4)
    return {
        "queries": draw_queries(jax.random.fold_in(arg_keys[3], 71), 0),
        "corpus": draw_corpus(jax.random.fold_in(arg_keys[3], 71), 0),
        "candidates": set_ends(jax.random.randint(arg_keys[2], (Q, K), 0, CORPUS), jax.random.fold_in(arg_keys[2], 1), 0, CORPUS - 1).astype(jnp.int32),
    }


def reference(queries, corpus, candidates):
    blocks = corpus.reshape(N_CORPUS, ROWS_DEV, D)

    def absorb(carry, block):
        peak, mass = carry
        scores = lax.dot_general(queries, block, (((1,), (1,)), ((), ())), preferred_element_type=jnp.float32)
        newer = jnp.maximum(peak, jnp.max(scores, axis=1))
        mass = mass * jnp.exp(peak - newer) + jnp.sum(jnp.exp(scores - newer[:, None]), axis=1)
        return (newer, mass), None

    start = (jnp.full((Q,), -1e30, jnp.float32), jnp.zeros((Q,), jnp.float32))
    (peak, mass), unused = lax.scan(absorb, start, blocks)
    lse = peak + jnp.log(mass)

    def score_query(packed):
        query, indices = packed
        chosen = jnp.take(corpus, indices.astype(jnp.int32), axis=0)
        return jnp.dot(chosen, query, preferred_element_type=jnp.float32)

    picked = lax.map(score_query, (queries, candidates))
    return picked - lse[:, None]
```

```python
import jax
import jax.numpy as jnp
from jax import lax
from jax.experimental import pallas as pl
from jax.experimental.pallas import tpu as pltpu
from jax.sharding import Mesh
from jax.sharding import PartitionSpec as P

CORPUS = ("corpus_0", "corpus_1", "corpus_2")
LANES = 128
LINES = 3


def lane_gather(table, lanes):
    return jnp.take_along_axis(table, lanes, axis=1, mode="promise_in_bounds")


def halves(queries, dim):
    half = queries.shape[1] // 2
    first, second = queries[:, :half], queries[:, half:]
    return jnp.where(dim == 0, first, second), jnp.where(dim == 0, second, first)


def matmul_nt(left, right):
    return lax.dot_general(left, right, (((1,), (1,)), ((), ())), preferred_element_type=jnp.float32)


def prepare(place_ref, queries_ref, corpus_ref, candidates_ref, partial_ref, theirs_ref, local_ref):
    mine, theirs_ref[...] = halves(queries_ref[...], place_ref[0])
    partial_ref[...] = matmul_nt(mine, corpus_ref[...])
    height = candidates_ref.shape[0]
    lane = lax.broadcasted_iota(jnp.int32, (height, LANES), 1)
    quarter = lane // (LANES // 4)
    for slot in range(4):
        source = 4 * (lane % (LANES // 4)) + slot
        for part in range(2):
            value = jnp.zeros((height, LANES), jnp.int32)
            for w in range(4):
                block = candidates_ref[:, pl.ds((4 * part + w) * LANES, LANES)]
                value = jnp.where(quarter == w, lane_gather(block, source), value)
            local_ref[:, pl.ds((2 * slot + part) * LANES, LANES)] = value - place_ref[1]


def pack(theirs_ref, other_ref, partial_ref, local_ref, out_ref):
    scores = partial_ref[...] + matmul_nt(theirs_ref[...], other_ref[...])
    height, count = scores.shape
    peak = jnp.max(scores, axis=1, keepdims=True)
    mass = jnp.sum(jnp.exp(scores - peak), axis=1, keepdims=True)

    def pick(column):
        local = local_ref[:, pl.ds(column * LANES, LANES)]
        block, lane = local >> 7, local & (LANES - 1)
        value = jnp.zeros((height, LANES), jnp.float32)
        for w in range(count // LANES):
            value = jnp.where(block == w, lane_gather(scores[:, w * LANES : (w + 1) * LANES], lane), value)
        return value

    for pair in range(2):
        for part in range(2):
            both = jnp.concatenate([pick(4 * pair + part), pick(4 * pair + 2 + part)], axis=0)
            out_ref[pl.ds(LANES * LINES * part + pair, LANES, stride=LINES), :] = both.T
    spread = jnp.concatenate([jnp.broadcast_to(peak, (height, LANES)), jnp.broadcast_to(mass, (height, LANES))], axis=0).T
    for part in range(2):
        out_ref[pl.ds(LANES * LINES * part + 2, LANES, stride=LINES), :] = spread


def finish(all_ref, out_ref):
    sources = all_ref.shape[0] // LINES
    stats = all_ref[pl.ds(2, sources, stride=LINES), :]
    peak = jnp.max(stats, axis=0, keepdims=True)
    mass = jnp.sum(jnp.exp(stats - peak) * pltpu.roll(stats, LANES // 2, 1), axis=0, keepdims=True)
    lse = (peak + jnp.log(mass))[:, : LANES // 2]
    for pair in range(2):
        picked = jnp.sum(all_ref[pl.ds(pair, sources, stride=LINES), :], axis=0, keepdims=True)
        out_ref[2 * pair : 2 * pair + 1, :] = picked[:, : LANES // 2] - lse
        out_ref[2 * pair + 1 : 2 * pair + 2, :] = picked[:, LANES // 2 :] - lse


VMEM = pl.BlockSpec(memory_space=pltpu.VMEM)
SMEM = pl.BlockSpec(memory_space=pltpu.SMEM)


def on_chip(value):
    return pltpu.with_memory_space_constraint(value, pltpu.VMEM)


def body(queries, corpus, candidates):
    rows, width = corpus.shape
    height, picks = candidates.shape
    size = lax.axis_size(CORPUS)
    place = jnp.stack([lax.axis_index("dim"), lax.axis_index(CORPUS) * rows]).astype(jnp.int32)
    other = lax.ppermute(corpus, "dim", [(0, 1), (1, 0)])
    partial, theirs, local = pl.pallas_call(
        prepare,
        out_shape=(
            pltpu.VMEM((height, rows), jnp.float32),
            pltpu.VMEM((height, width), queries.dtype),
            pltpu.VMEM((height, picks), jnp.int32),
        ),
        in_specs=[SMEM, VMEM, VMEM, VMEM],
        out_specs=(VMEM, VMEM, VMEM),
        cost_estimate=pl.CostEstimate(flops=2 * height * rows * width, bytes_accessed=2 * rows * width, transcendentals=0),
        name="prepare",
    )(place, queries, corpus, candidates)
    sent = pl.pallas_call(
        pack,
        out_shape=pltpu.VMEM((size * LINES, LANES), jnp.float32),
        in_specs=[VMEM, VMEM, VMEM, VMEM],
        out_specs=VMEM,
        name="pack",
    )(on_chip(theirs), on_chip(other), on_chip(partial), on_chip(local))
    arrived = lax.all_to_all(sent.reshape(size, 1, LINES * LANES), CORPUS, split_axis=0, concat_axis=0, tiled=True)
    out = pl.pallas_call(
        finish,
        out_shape=jax.ShapeDtypeStruct((picks // size, height), jnp.float32),
        in_specs=[VMEM],
        out_specs=VMEM,
        name="finish",
    )(on_chip(arrived.reshape(size * LINES, LANES)))
    return out.T


def solution(mesh):
    torus = Mesh(
        mesh.devices.reshape(8, 8, 4, mesh.shape["dim"]),
        (*CORPUS, "dim"),
    )
    return jax.shard_map(
        body,
        mesh=torus,
        in_specs=(P("dim", None), P(CORPUS, "dim"), P("dim", None)),
        out_specs=P("dim", CORPUS),
        check_vma=False,
    )
```

```python
import jax
import jax.numpy as jnp
from jax import lax
from jax.experimental import pallas as pl
from jax.experimental.pallas import tpu as pltpu
from jax.sharding import Mesh
from jax.sharding import PartitionSpec as P

CORPUS = ("corpus_0", "corpus_1", "corpus_2")
LANES = 128
HALF = LANES // 2
LINES = 4


def lane_gather(table, lanes):
    return jnp.take_along_axis(table, lanes, axis=1, mode="promise_in_bounds")


def halves(queries, dim):
    half = queries.shape[1] // 2
    first, second = queries[:, :half], queries[:, half:]
    return jnp.where(dim == 0, first, second), jnp.where(dim == 0, second, first)


def matmul_nt(left, right):
    return lax.dot_general(left, right, (((1,), (1,)), ((), ())), preferred_element_type=jnp.float32)


def spread(column):
    return jnp.broadcast_to(column, (column.shape[0], LANES))


def rounded(value):
    return value.astype(jnp.bfloat16).astype(jnp.float32)


def prepare(queries_ref, corpus_ref, candidates_ref, partial_ref, theirs_ref, local_ref, owner_ref):
    mine, theirs_ref[...] = halves(queries_ref[...], lax.axis_index("dim"))
    partial_ref[...] = matmul_nt(mine, corpus_ref[...])
    height = candidates_ref.shape[0]
    rows = corpus_ref.shape[0]
    position = lax.axis_index(CORPUS)
    lane = lax.broadcasted_iota(jnp.int32, (height, LANES), 1)
    group = LANES // 4
    quarter = lane // group
    for slot in range(4):
        source = 4 * (lane % group) + slot
        for part in range(2):
            value = jnp.zeros((height, LANES), jnp.int32)
            for w in range(4):
                block = candidates_ref[:, pl.ds((4 * part + w) * LANES, LANES)]
                value = jnp.where(quarter == w, lane_gather(block, source), value)
            local_ref[:, pl.ds((2 * slot + part) * LANES, LANES)] = value - position * rows
    own = candidates_ref[:, pl.ds(pl.multiple_of(position // group * LANES, LANES), LANES)]
    at = jnp.full((height, LANES), 4 * (position % group), jnp.int32)
    for pair in range(2):
        both = jnp.concatenate([lane_gather(own, at + 2 * pair), lane_gather(own, at + 2 * pair + 1)], axis=0)
        owner_ref[pair : pair + 1, :] = (both.astype(jnp.float32).T)[:1, :].astype(jnp.int32) // rows


def pack(theirs_ref, other_ref, partial_ref, local_ref, out_ref, lines_ref):
    scores = partial_ref[...] + matmul_nt(theirs_ref[...], other_ref[...])
    height, count = scores.shape
    peak = jnp.max(scores, axis=1, keepdims=True)
    lse = peak + jnp.log(jnp.sum(jnp.exp(scores - peak), axis=1, keepdims=True))
    center = rounded(jnp.sum(scores, axis=1, keepdims=True) * (1.0 / count))
    moved = scores - center

    def pick(column):
        local = local_ref[:, pl.ds(column * LANES, LANES)]
        block, lane = local >> 7, local & (LANES - 1)
        value = jnp.zeros((height, LANES), jnp.float32)
        for w in range(count // LANES):
            value = jnp.where(block == w, lane_gather(moved[:, w * LANES : (w + 1) * LANES], lane), value)
        return value

    def write(line, part, value):
        lines_ref[pl.ds(LANES * LINES * part + line, LANES, stride=LINES), :] = value

    for pair in range(2):
        for part in range(2):
            both = jnp.concatenate([pick(4 * pair + part), pick(4 * pair + 2 + part)], axis=0)
            write(pair, part, both.T)
    upper = rounded(lse)
    middle = rounded(lse - upper)
    lower = lse - upper - middle
    first = jnp.concatenate([spread(upper), spread(middle)], axis=0).T
    second = jnp.concatenate([spread(lower), spread(center)], axis=0).T
    for part in range(2):
        write(2, part, first)
        write(3, part, second)
    out_ref[...] = lines_ref[...].astype(jnp.bfloat16)


def finish(all_ref, owner_ref, out_ref, lines_ref):
    lines_ref[...] = all_ref[...].astype(jnp.float32)
    sources = all_ref.shape[0] // LINES
    first = lines_ref[pl.ds(2, sources, stride=LINES), :]
    second = lines_ref[pl.ds(3, sources, stride=LINES), :]
    local = first + pltpu.roll(first, HALF, 1) + second
    low = lax.broadcasted_iota(jnp.int32, (1, LANES), 1) < HALF
    peak = jnp.max(local, axis=0, keepdims=True)
    mass = jnp.sum(jnp.exp(local - peak), axis=0, keepdims=True)
    lse = (peak + jnp.log(mass))[:, :HALF]
    center = jnp.where(low, pltpu.roll(second, HALF, 1), second)
    source = lax.broadcasted_iota(jnp.int32, (sources, LANES), 0)
    for pair in range(2):
        moved = lines_ref[pl.ds(pair, sources, stride=LINES), :]
        back = jnp.where(source == owner_ref[pair : pair + 1, :], center, 0.0)
        picked = jnp.sum(moved + back, axis=0, keepdims=True)
        out_ref[2 * pair : 2 * pair + 1, :] = picked[:, :HALF] - lse
        out_ref[2 * pair + 1 : 2 * pair + 2, :] = picked[:, HALF:] - lse


VMEM = pl.BlockSpec(memory_space=pltpu.VMEM)


def on_chip(value):
    return pltpu.with_memory_space_constraint(value, pltpu.VMEM)


def body(queries, corpus, candidates):
    rows, width = corpus.shape
    height, picks = candidates.shape
    size = lax.axis_size(CORPUS)
    other = lax.ppermute(corpus, "dim", [(0, 1), (1, 0)])
    partial, theirs, local, owner = pl.pallas_call(
        prepare,
        out_shape=(
            pltpu.VMEM((height, rows), jnp.float32),
            pltpu.VMEM((height, width), queries.dtype),
            pltpu.VMEM((height, picks), jnp.int32),
            pltpu.VMEM((2, LANES), jnp.int32),
        ),
        in_specs=[VMEM, VMEM, VMEM],
        out_specs=(VMEM, VMEM, VMEM, VMEM),
        cost_estimate=pl.CostEstimate(flops=2 * height * rows * width, bytes_accessed=2 * rows * width, transcendentals=0),
        name="prepare",
    )(queries, corpus, candidates)
    sent = pl.pallas_call(
        pack,
        out_shape=pltpu.VMEM((size * LINES, LANES), jnp.bfloat16),
        in_specs=[VMEM, VMEM, VMEM, VMEM],
        out_specs=VMEM,
        scratch_shapes=[pltpu.VMEM((size * LINES, LANES), jnp.float32)],
        name="pack",
    )(on_chip(theirs), on_chip(other), on_chip(partial), on_chip(local))
    arrived = lax.all_to_all(sent.reshape(size, LINES, LANES), CORPUS, split_axis=0, concat_axis=0, tiled=True)
    out = pl.pallas_call(
        finish,
        out_shape=jax.ShapeDtypeStruct((picks // size, height), jnp.float32),
        in_specs=[VMEM, VMEM],
        out_specs=VMEM,
        scratch_shapes=[pltpu.VMEM((size * LINES, LANES), jnp.float32)],
        name="finish",
    )(on_chip(arrived.reshape(size * LINES, LANES)), on_chip(owner))
    return out.T


def solution(mesh):
    torus = Mesh(
        mesh.devices.reshape(8, 8, 4, mesh.shape["dim"]),
        (*CORPUS, "dim"),
    )
    return jax.shard_map(
        body,
        mesh=torus,
        in_specs=(P("dim", None), P(CORPUS, "dim"), P("dim", None)),
        out_specs=P("dim", CORPUS),
        check_vma=False,
    )
```

```python
import functools

import jax
import jax.numpy as jnp
from jax import lax
from jax.experimental import pallas as pl
from jax.experimental.pallas import tpu as pltpu
from jax.sharding import Mesh
from jax.sharding import PartitionSpec as P

CORPUS = ("corpus_0", "corpus_1", "corpus_2")
LANES = 128
HALF = LANES // 2
LINES = 4
FIRST = (4, 4, 2)


def first_rank(shape):
    position = 0
    for at, size in zip(FIRST, shape):
        position = position * size + at
    return position


def lane_gather(table, lanes):
    return jnp.take_along_axis(table, lanes, axis=1, mode="promise_in_bounds")


def halves(queries, dim):
    half = queries.shape[1] // 2
    first, second = queries[:, :half], queries[:, half:]
    return jnp.where(dim == 0, first, second), jnp.where(dim == 0, second, first)


def matmul_nt(left, right):
    return lax.dot_general(left, right, (((1,), (1,)), ((), ())), preferred_element_type=jnp.float32)


def spread(column):
    return jnp.broadcast_to(column, (column.shape[0], LANES))


def rounded(value):
    return value.astype(jnp.bfloat16).astype(jnp.float32)


def prepare(first, queries_ref, corpus_ref, candidates_ref, partial_ref, theirs_ref, local_ref, owner_ref):
    mine, theirs_ref[...] = halves(queries_ref[...], lax.axis_index("dim"))
    partial_ref[...] = matmul_nt(mine, corpus_ref[...])
    height = candidates_ref.shape[0]
    rows = corpus_ref.shape[0]
    position = lax.axis_index(CORPUS)
    lane = lax.broadcasted_iota(jnp.int32, (height, LANES), 1) ^ (first % LANES)
    group = LANES // 4
    quarter = lane // group
    for slot in range(4):
        source = 4 * (lane % group) + slot
        for part in range(2):
            value = jnp.zeros((height, LANES), jnp.int32)
            for w in range(4):
                block = candidates_ref[:, pl.ds((4 * (part ^ (first // LANES)) + w) * LANES, LANES)]
                value = jnp.where(quarter == w, lane_gather(block, source), value)
            local_ref[:, pl.ds((2 * slot + part) * LANES, LANES)] = value - position * rows
    own = candidates_ref[:, pl.ds(pl.multiple_of(position // group * LANES, LANES), LANES)]
    at = jnp.full((height, LANES), 4 * (position % group), jnp.int32)
    for pair in range(2):
        both = jnp.concatenate([lane_gather(own, at + 2 * pair), lane_gather(own, at + 2 * pair + 1)], axis=0)
        owner_ref[pair : pair + 1, :] = ((both.astype(jnp.float32).T)[:1, :].astype(jnp.int32) // rows) ^ first


def pack(theirs_ref, other_ref, partial_ref, local_ref, out_ref, lines_ref):
    scores = partial_ref[...] + matmul_nt(theirs_ref[...], other_ref[...])
    height, count = scores.shape
    peak = jnp.max(scores, axis=1, keepdims=True)
    lse = peak + jnp.log(jnp.sum(jnp.exp(scores - peak), axis=1, keepdims=True))
    center = rounded(jnp.sum(scores, axis=1, keepdims=True) * (1.0 / count))
    moved = scores - center

    def pick(column):
        local = local_ref[:, pl.ds(column * LANES, LANES)]
        block, lane = local >> 7, local & (LANES - 1)
        value = jnp.zeros((height, LANES), jnp.float32)
        for w in range(count // LANES):
            value = jnp.where(block == w, lane_gather(moved[:, w * LANES : (w + 1) * LANES], lane), value)
        return value

    def write(line, part, value):
        lines_ref[pl.ds(LANES * LINES * part + line, LANES, stride=LINES), :] = value

    for pair in range(2):
        for part in range(2):
            both = jnp.concatenate([pick(4 * pair + part), pick(4 * pair + 2 + part)], axis=0)
            write(pair, part, both.T)
    upper = rounded(lse)
    middle = rounded(lse - upper)
    lower = lse - upper - middle
    first = jnp.concatenate([spread(upper), spread(middle)], axis=0).T
    second = jnp.concatenate([spread(lower), spread(center)], axis=0).T
    for part in range(2):
        write(2, part, first)
        write(3, part, second)
    out_ref[...] = lines_ref[...].astype(jnp.bfloat16)


def finish(all_ref, owner_ref, out_ref, lines_ref):
    lines_ref[...] = all_ref[...].astype(jnp.float32)
    sources = all_ref.shape[0] // LINES
    first = lines_ref[pl.ds(2, sources, stride=LINES), :]
    second = lines_ref[pl.ds(3, sources, stride=LINES), :]
    local = first + pltpu.roll(first, HALF, 1) + second
    low = lax.broadcasted_iota(jnp.int32, (1, LANES), 1) < HALF
    peak = jnp.max(local, axis=0, keepdims=True)
    mass = jnp.sum(jnp.exp(local - peak), axis=0, keepdims=True)
    lse = (peak + jnp.log(mass))[:, :HALF]
    center = jnp.where(low, pltpu.roll(second, HALF, 1), second)
    source = lax.broadcasted_iota(jnp.int32, (sources, LANES), 0)
    for pair in range(2):
        moved = lines_ref[pl.ds(pair, sources, stride=LINES), :]
        back = jnp.where(source == owner_ref[pair : pair + 1, :], center, 0.0)
        picked = jnp.sum(moved + back, axis=0, keepdims=True)
        out_ref[2 * pair : 2 * pair + 1, :] = picked[:, :HALF] - lse
        out_ref[2 * pair + 1 : 2 * pair + 2, :] = picked[:, HALF:] - lse


VMEM = pl.BlockSpec(memory_space=pltpu.VMEM)


def on_chip(value):
    return pltpu.with_memory_space_constraint(value, pltpu.VMEM)


def body(queries, corpus, candidates):
    rows, width = corpus.shape
    height, picks = candidates.shape
    size = lax.axis_size(CORPUS)
    first = first_rank([lax.axis_size(axis) for axis in CORPUS])
    other = lax.ppermute(corpus, "dim", [(0, 1), (1, 0)])
    partial, theirs, local, owner = pl.pallas_call(
        functools.partial(prepare, first),
        out_shape=(
            pltpu.VMEM((height, rows), jnp.float32),
            pltpu.VMEM((height, width), queries.dtype),
            pltpu.VMEM((height, picks), jnp.int32),
            pltpu.VMEM((2, LANES), jnp.int32),
        ),
        in_specs=[VMEM, VMEM, VMEM],
        out_specs=(VMEM, VMEM, VMEM, VMEM),
        cost_estimate=pl.CostEstimate(flops=2 * height * rows * width, bytes_accessed=2 * rows * width, transcendentals=0),
        name="prepare",
    )(queries, corpus, candidates)
    sent = pl.pallas_call(
        pack,
        out_shape=pltpu.VMEM((size * LINES, LANES), jnp.bfloat16),
        in_specs=[VMEM, VMEM, VMEM, VMEM],
        out_specs=VMEM,
        scratch_shapes=[pltpu.VMEM((size * LINES, LANES), jnp.float32)],
        name="pack",
    )(on_chip(theirs), on_chip(other), on_chip(partial), on_chip(local))
    ranks = [[rank ^ first for rank in range(size)]]
    arrived = lax.all_to_all(
        sent.reshape(size, LINES, LANES), CORPUS, split_axis=0, concat_axis=0, axis_index_groups=ranks, tiled=True
    )
    out = pl.pallas_call(
        finish,
        out_shape=jax.ShapeDtypeStruct((picks // size, height), jnp.float32),
        in_specs=[VMEM, VMEM],
        out_specs=VMEM,
        scratch_shapes=[pltpu.VMEM((size * LINES, LANES), jnp.float32)],
        name="finish",
    )(on_chip(arrived.reshape(size * LINES, LANES)), on_chip(owner))
    return out.T


def solution(mesh):
    torus = Mesh(
        mesh.devices.reshape(8, 8, 4, mesh.shape["dim"]),
        (*CORPUS, "dim"),
    )
    return jax.shard_map(
        body,
        mesh=torus,
        in_specs=(P("dim", None), P(CORPUS, "dim"), P("dim", None)),
        out_specs=P("dim", CORPUS),
        check_vma=False,
    )
```

```python
import functools

import jax
import jax.numpy as jnp
from jax import lax
from jax.experimental import pallas as pl
from jax.experimental.pallas import tpu as pltpu
from jax.sharding import Mesh
from jax.sharding import PartitionSpec as P

CORPUS = ("corpus_0", "corpus_1", "corpus_2")
LANES = 128
HALF = LANES // 2
GROUP = LANES // 4
LINES = 4
FIRST = (4, 4, 2)


def first_rank(shape):
    position = 0
    for at, size in zip(FIRST, shape):
        position = position * size + at
    return position


def lane_gather(table, lanes):
    numbers = lax.GatherDimensionNumbers(
        offset_dims=(),
        collapsed_slice_dims=(1,),
        start_index_map=(1,),
        operand_batching_dims=(0,),
        start_indices_batching_dims=(0,),
    )
    return lax.gather(
        table, lanes[:, :, None], numbers, slice_sizes=(1, 1), mode=lax.GatherScatterMode.PROMISE_IN_BOUNDS
    )


def halves(queries, dim):
    half = queries.shape[1] // 2
    first, second = queries[:, :half], queries[:, half:]
    return jnp.where(dim == 0, first, second), jnp.where(dim == 0, second, first)


def matmul_nt(left, right):
    return lax.dot_general(left, right, (((1,), (1,)), ((), ())), preferred_element_type=jnp.float32)


def rounded(value):
    return value.astype(jnp.bfloat16).astype(jnp.float32)


def prepare(
    first,
    queries_in,
    corpus_in,
    candidates_in,
    partial_ref,
    theirs_ref,
    local_ref,
    owner_ref,
    order_ref,
    queries_ref,
    corpus_ref,
    candidates_ref,
    arrived,
):
    loads = [
        pltpu.make_async_copy(source, target, arrived.at[k])
        for k, (source, target) in enumerate(
            [(candidates_in, candidates_ref), (queries_in, queries_ref), (corpus_in, corpus_ref)]
        )
    ]
    for load in loads:
        load.start()
    row = lax.broadcasted_iota(jnp.int32, (2 * LANES, 1), 0)
    line = row % LINES
    taken = jnp.where(line < 2, row // LANES * HALF + line * GROUP + row % LANES // LINES, LANES + (line - 2) * HALF)
    column = lax.broadcasted_iota(jnp.int32, (2 * LANES, 2 * LANES), 1)
    order_ref[...] = jnp.where(column == taken, 1.0, 0.0).astype(jnp.bfloat16)
    height = candidates_ref.shape[0]
    rows = corpus_ref.shape[0]
    position = lax.axis_index(CORPUS)
    lane = lax.broadcasted_iota(jnp.int32, (height, LANES), 1)
    loads[0].wait()
    for side in range(2):
        source = 4 * ((lane % GROUP) ^ (first % GROUP)) + 2 * (lane % HALF // GROUP) + side
        for pair in range(4):
            low, high = [
                lane_gather(candidates_ref[:, pl.ds(((2 * pair + k) ^ (first // GROUP)) * LANES, LANES)], source)
                for k in range(2)
            ]
            local_ref[:, pl.ds((2 * pair + side) * LANES, LANES)] = jnp.where(lane < HALF, low, high) - position * rows
    own = candidates_ref[:, pl.ds(pl.multiple_of(position // GROUP * LANES, LANES), LANES)]
    at = jnp.full((height, LANES), 4 * (position % GROUP), jnp.int32)
    for line in range(2):
        both = jnp.concatenate([lane_gather(own, at + 2 * line), lane_gather(own, at + 2 * line + 1)], axis=0)
        owner_ref[line : line + 1, :] = ((both.astype(jnp.float32).T)[:1, :].astype(jnp.int32) // rows) ^ first
    loads[1].wait()
    mine, theirs_ref[...] = halves(queries_ref[...], lax.axis_index("dim"))
    loads[2].wait()
    partial_ref[...] = matmul_nt(mine, corpus_ref[...])


def pack(theirs_ref, other_ref, partial_ref, local_ref, order_ref, out_ref):
    scores = partial_ref[...] + matmul_nt(theirs_ref[...], other_ref[...])
    height, count = scores.shape
    peak = jnp.max(scores, axis=1, keepdims=True)
    lse = peak + jnp.log(jnp.sum(jnp.exp(scores - peak), axis=1, keepdims=True))
    center = rounded(jnp.sum(scores, axis=1, keepdims=True) * (1.0 / count))
    moved = scores - center
    upper = rounded(lse)
    middle = rounded(lse - upper)
    lower = lse - upper - middle
    low = lax.broadcasted_iota(jnp.int32, (height, LANES), 1) < HALF
    stats = jnp.concatenate([jnp.where(low, upper, lower), jnp.where(low, middle, center)], axis=0).astype(jnp.bfloat16)

    blocks = count // LANES
    parts = [[] for _ in range(8)]
    for top in range(0, height, 8):
        for column in range(8):
            local = local_ref[top : top + 8, pl.ds(column * LANES, LANES)]
            block, lane = local >> 7, local & (LANES - 1)
            value = jnp.zeros((8, LANES), jnp.float32)
            for w in range(blocks):
                table = moved[top : top + 8, w * LANES : (w + 1) * LANES]
                value = jnp.where(block == w, lane_gather(table, lane), value)
            parts[column].append(value)
    picked = [jnp.concatenate(part, axis=0) for part in parts]
    for pair in range(4):
        both = jnp.concatenate([picked[2 * pair], picked[2 * pair + 1]], axis=0).astype(jnp.bfloat16)
        lines = matmul_nt(order_ref[...], jnp.concatenate([both, stats], axis=1))
        out_ref[pl.ds(2 * LANES * pair, 2 * LANES), :] = lines.astype(jnp.bfloat16)


def finish(all_ref, owner_ref, out_ref, lines_ref):
    lines_ref[...] = all_ref[...].astype(jnp.float32)
    sources = all_ref.shape[0] // LINES
    first = lines_ref[pl.ds(2, sources, stride=LINES), :]
    second = lines_ref[pl.ds(3, sources, stride=LINES), :]
    local = first + pltpu.roll(first, HALF, 1) + second
    low = lax.broadcasted_iota(jnp.int32, (1, LANES), 1) < HALF
    peak = jnp.max(local, axis=0, keepdims=True)
    mass = jnp.sum(jnp.exp(local - peak), axis=0, keepdims=True)
    lse = (peak + jnp.log(mass))[:, :HALF]
    center = jnp.where(low, pltpu.roll(second, HALF, 1), second)
    source = lax.broadcasted_iota(jnp.int32, (sources, LANES), 0)
    for pair in range(2):
        moved = lines_ref[pl.ds(pair, sources, stride=LINES), :]
        back = jnp.where(source == owner_ref[pair : pair + 1, :], center, 0.0)
        picked = jnp.sum(moved + back, axis=0, keepdims=True)
        out_ref[2 * pair : 2 * pair + 1, :] = picked[:, :HALF] - lse
        out_ref[2 * pair + 1 : 2 * pair + 2, :] = picked[:, HALF:] - lse


VMEM = pl.BlockSpec(memory_space=pltpu.VMEM)
ANY = pl.BlockSpec(memory_space=pl.ANY)


def on_chip(value):
    return pltpu.with_memory_space_constraint(value, pltpu.VMEM)


def body(queries, corpus, candidates):
    rows, width = corpus.shape
    height, picks = candidates.shape
    size = lax.axis_size(CORPUS)
    first = first_rank([lax.axis_size(axis) for axis in CORPUS])
    other = lax.ppermute(corpus, "dim", [(0, 1), (1, 0)])
    partial, theirs, local, owner, order = pl.pallas_call(
        functools.partial(prepare, first),
        out_shape=(
            pltpu.VMEM((height, rows), jnp.float32),
            pltpu.VMEM((height, width), queries.dtype),
            pltpu.VMEM((height, picks), jnp.int32),
            pltpu.VMEM((2, LANES), jnp.int32),
            pltpu.VMEM((2 * LANES, 2 * LANES), jnp.bfloat16),
        ),
        in_specs=[ANY, ANY, ANY],
        out_specs=(VMEM, VMEM, VMEM, VMEM, VMEM),
        scratch_shapes=[
            pltpu.VMEM(queries.shape, queries.dtype),
            pltpu.VMEM(corpus.shape, corpus.dtype),
            pltpu.VMEM(candidates.shape, candidates.dtype),
            pltpu.SemaphoreType.DMA((3,)),
        ],
        cost_estimate=pl.CostEstimate(flops=2 * height * rows * width, bytes_accessed=2 * rows * width, transcendentals=0),
        name="prepare",
    )(queries, corpus, candidates)
    sent = pl.pallas_call(
        pack,
        out_shape=pltpu.VMEM((size * LINES, LANES), jnp.bfloat16),
        in_specs=[VMEM, VMEM, VMEM, VMEM, VMEM],
        out_specs=VMEM,
        name="pack",
    )(on_chip(theirs), on_chip(other), on_chip(partial), on_chip(local), on_chip(order))
    ranks = [[rank ^ first for rank in range(size)]]
    arrived = lax.all_to_all(
        sent.reshape(size, LINES, LANES), CORPUS, split_axis=0, concat_axis=0, axis_index_groups=ranks, tiled=True
    )
    out = pl.pallas_call(
        finish,
        out_shape=jax.ShapeDtypeStruct((picks // size, height), jnp.float32),
        in_specs=[VMEM, VMEM],
        out_specs=VMEM,
        scratch_shapes=[pltpu.VMEM((size * LINES, LANES), jnp.float32)],
        name="finish",
    )(on_chip(arrived.reshape(size * LINES, LANES)), on_chip(owner))
    return out.T


def solution(mesh):
    torus = Mesh(
        mesh.devices.reshape(8, 8, 4, mesh.shape["dim"]),
        (*CORPUS, "dim"),
    )
    return jax.shard_map(
        body,
        mesh=torus,
        in_specs=(P("dim", None), P(CORPUS, "dim"), P("dim", None)),
        out_specs=P("dim", CORPUS),
        check_vma=False,
    )
```

```python
import functools

import jax
import jax.numpy as jnp
from jax import lax
from jax.experimental import pallas as pl
from jax.experimental.pallas import tpu as pltpu
from jax.sharding import Mesh
from jax.sharding import PartitionSpec as P

CORPUS = ("corpus_0", "corpus_1", "corpus_2")
LANES = 128
HALF = LANES // 2
GROUP = LANES // 4
LINES = 4
TINY = 1e-30
FIRST = (4, 4, 2)


def first_rank(shape):
    position = 0
    for at, size in zip(FIRST, shape):
        position = position * size + at
    return position


def lane_gather(table, lanes):
    numbers = lax.GatherDimensionNumbers(
        offset_dims=(),
        collapsed_slice_dims=(1,),
        start_index_map=(1,),
        operand_batching_dims=(0,),
        start_indices_batching_dims=(0,),
    )
    return lax.gather(
        table, lanes[:, :, None], numbers, slice_sizes=(1, 1), mode=lax.GatherScatterMode.PROMISE_IN_BOUNDS
    )


def matmul_nt(left, right):
    return lax.dot_general(left, right, (((1,), (1,)), ((), ())), preferred_element_type=jnp.float32)


def rounded(value):
    return value.astype(jnp.bfloat16).astype(jnp.float32)


def message_order(first):
    row = lax.broadcasted_iota(jnp.int32, (LANES, LANES), 0)
    lane = lax.broadcasted_iota(jnp.int32, (LANES, LANES), 1)
    line = row % LINES
    slot = LINES * (row // LINES ^ (first % GROUP)) + 2 * line
    picks = line < 2
    hits = [picks & (lane == slot), picks & (lane == slot + 1), lane == (line - 2) * HALF]
    return jnp.concatenate([jnp.where(hit, 1.0, 0.0).astype(jnp.bfloat16) for hit in hits], axis=1)


def pack(first, queries_ref, corpus_ref, candidates_ref, out_ref):
    width = corpus_ref.shape[2]
    scores = matmul_nt(queries_ref[:, :width], corpus_ref[0]) + matmul_nt(queries_ref[:, width:], corpus_ref[1])
    height, count = scores.shape
    order = message_order(first)
    peak = jnp.max(scores, axis=1, keepdims=True)
    lse = peak + jnp.log(jnp.sum(jnp.exp(scores - peak), axis=1, keepdims=True))
    center = rounded(jnp.sum(scores, axis=1, keepdims=True) * (1.0 / count))
    moved = scores - center
    moved = jnp.where(jnp.abs(moved) < TINY, TINY, moved)
    upper = rounded(lse)
    middle = rounded(lse - upper)
    lower = lse - upper - middle
    low = lax.broadcasted_iota(jnp.int32, (height, LANES), 1) < HALF
    stats = jnp.concatenate([jnp.where(low, upper, lower), jnp.where(low, middle, center)], axis=0).astype(jnp.bfloat16)
    offset = lax.axis_index(CORPUS) * count
    nothing = jnp.zeros((height, LANES), jnp.bfloat16)
    for tile in range(candidates_ref.shape[1] // LANES):
        local = candidates_ref[:, tile * LANES : (tile + 1) * LANES] - offset
        block, lane = local >> 7, local & (LANES - 1)
        value = jnp.zeros((height, LANES), jnp.float32)
        for w in range(count // LANES):
            value = jnp.where(block == w, lane_gather(moved[:, w * LANES : (w + 1) * LANES], lane), value)
        value = value.astype(jnp.bfloat16)
        both = jnp.concatenate(
            [jnp.concatenate([value, nothing], axis=0), jnp.concatenate([nothing, value], axis=0), stats], axis=1
        )
        group = tile ^ (first // GROUP)
        out_ref[group * LANES : (group + 1) * LANES, :] = matmul_nt(order, both).astype(jnp.bfloat16)


def finish(all_ref, out_ref, lines_ref):
    lines_ref[...] = all_ref[...].astype(jnp.float32)
    sources = all_ref.shape[0] // LINES
    first = lines_ref[pl.ds(2, sources, stride=LINES), :]
    second = lines_ref[pl.ds(3, sources, stride=LINES), :]
    local = first + pltpu.roll(first, HALF, 1) + second
    low = lax.broadcasted_iota(jnp.int32, (1, LANES), 1) < HALF
    peak = jnp.max(local, axis=0, keepdims=True)
    mass = jnp.sum(jnp.exp(local - peak), axis=0, keepdims=True)
    lse = (peak + jnp.log(mass))[:, :HALF]
    center = jnp.where(low, pltpu.roll(second, HALF, 1), second)
    for pair in range(2):
        moved = lines_ref[pl.ds(pair, sources, stride=LINES), :]
        picked = jnp.sum(jnp.where(moved != 0.0, moved + center, 0.0), axis=0, keepdims=True)
        out_ref[2 * pair : 2 * pair + 1, :] = picked[:, :HALF] - lse
        out_ref[2 * pair + 1 : 2 * pair + 2, :] = picked[:, HALF:] - lse


VMEM = pl.BlockSpec(memory_space=pltpu.VMEM)


def on_chip(value):
    return pltpu.with_memory_space_constraint(value, pltpu.VMEM)


def body(queries, corpus, candidates):
    height, picks = candidates.shape
    size = lax.axis_size(CORPUS)
    first = first_rank([lax.axis_size(axis) for axis in CORPUS])
    both = lax.all_gather(corpus, "dim")
    sent = pl.pallas_call(
        functools.partial(pack, first),
        out_shape=pltpu.VMEM((size * LINES, LANES), jnp.bfloat16),
        in_specs=[VMEM, VMEM, VMEM],
        out_specs=VMEM,
        name="pack",
    )(on_chip(queries), on_chip(both), on_chip(candidates))
    ranks = [[rank ^ first for rank in range(size)]]
    arrived = lax.all_to_all(
        sent.reshape(size, LINES, LANES), CORPUS, split_axis=0, concat_axis=0, axis_index_groups=ranks, tiled=True
    )
    out = pl.pallas_call(
        finish,
        out_shape=jax.ShapeDtypeStruct((picks // size, height), jnp.float32),
        in_specs=[VMEM],
        out_specs=VMEM,
        scratch_shapes=[pltpu.VMEM((size * LINES, LANES), jnp.float32)],
        name="finish",
    )(on_chip(arrived.reshape(size * LINES, LANES)))
    return out.T


def solution(mesh):
    torus = Mesh(
        mesh.devices.reshape(8, 8, 4, mesh.shape["dim"]),
        (*CORPUS, "dim"),
    )
    return jax.shard_map(
        body,
        mesh=torus,
        in_specs=(P("dim", None), P(CORPUS, "dim"), P("dim", None)),
        out_specs=P("dim", CORPUS),
        check_vma=False,
    )
```

```python
import functools

import jax
import jax.numpy as jnp
from jax import lax
from jax.experimental import pallas as pl
from jax.experimental.pallas import tpu as pltpu
from jax.sharding import Mesh
from jax.sharding import PartitionSpec as P

CORPUS = ("corpus_0", "corpus_1", "corpus_2")
LANES = 128
HALF = LANES // 2
LINES = 4
RING = 4
TILE = 16
MESSAGE = LANES + TILE
TINY = 1e-30
FIRST = (4, 4, 2)


def first_rank(shape):
    position = 0
    for at, size in zip(FIRST, shape):
        position = position * size + at
    return position


def lane_gather(table, lanes):
    numbers = lax.GatherDimensionNumbers(
        offset_dims=(),
        collapsed_slice_dims=(1,),
        start_index_map=(1,),
        operand_batching_dims=(0,),
        start_indices_batching_dims=(0,),
    )
    return lax.gather(
        table, lanes[:, :, None], numbers, slice_sizes=(1, 1), mode=lax.GatherScatterMode.PROMISE_IN_BOUNDS
    )


def matmul_nt(left, right):
    return lax.dot_general(left, right, (((1,), (1,)), ((), ())), preferred_element_type=jnp.float32)


def kept_off_zero(value):
    return jnp.where(jnp.abs(value) < TINY, TINY, value)


def rounded(value):
    return value.astype(jnp.bfloat16).astype(jnp.float32)


def ones_where(hit):
    return jnp.where(hit, 1.0, 0.0).astype(jnp.bfloat16)


def ring_order(first):
    row = lax.broadcasted_iota(jnp.int32, (HALF, LANES), 0)
    lane = lax.broadcasted_iota(jnp.int32, (HALF, LANES), 1)
    near = row // TILE ^ (first % RING)
    far = row % TILE // 2 ^ (first // RING % 8)
    slot = TILE * far + 4 * near + 2 * (row % 2)
    return jnp.concatenate([ones_where(lane == slot), ones_where(lane == slot + 1)], axis=1)


def pack(first, queries_ref, corpus_ref, candidates_ref, out_ref):
    width = corpus_ref.shape[2]
    scores = matmul_nt(queries_ref[:, :width], corpus_ref[0]) + matmul_nt(queries_ref[:, width:], corpus_ref[1])
    height, count = scores.shape
    order = ring_order(first)
    peak = jnp.max(scores, axis=1, keepdims=True)
    lse = peak + jnp.log(jnp.sum(jnp.exp(scores - peak), axis=1, keepdims=True))
    center = rounded(jnp.sum(scores, axis=1, keepdims=True) * (1.0 / count))
    moved = kept_off_zero(scores - center)
    upper = rounded(lse)
    middle = rounded(lse - upper)
    lower = lse - upper - middle
    low = lax.broadcasted_iota(jnp.int32, (height, LANES), 1) < HALF
    stats = jnp.concatenate([jnp.where(low, upper, lower), jnp.where(low, middle, center)], axis=0).astype(jnp.bfloat16)
    offset = lax.axis_index(CORPUS) * count
    nothing = jnp.zeros((height, LANES), jnp.bfloat16)
    for tile in range(candidates_ref.shape[1] // LANES):
        local = candidates_ref[:, tile * LANES : (tile + 1) * LANES] - offset
        block, lane = local >> 7, local & (LANES - 1)
        value = jnp.zeros((height, LANES), jnp.float32)
        for w in range(count // LANES):
            value = jnp.where(block == w, lane_gather(moved[:, w * LANES : (w + 1) * LANES], lane), value)
        value = value.astype(jnp.bfloat16)
        both = jnp.concatenate(
            [jnp.concatenate([value, nothing], axis=0), jnp.concatenate([nothing, value], axis=0)], axis=1
        )
        lines = matmul_nt(order, both).astype(jnp.bfloat16)
        at = TILE * (tile ^ (first // RING // 8))
        for near in range(RING):
            out_ref[near * MESSAGE + at : near * MESSAGE + at + TILE, :] = lines[near * TILE : (near + 1) * TILE]
    row = lax.broadcasted_iota(jnp.int32, (TILE, LANES), 0)
    lane = lax.broadcasted_iota(jnp.int32, (TILE, LANES), 1)
    last = matmul_nt(ones_where((row < 2) & (lane == row * HALF)), stats).astype(jnp.bfloat16)
    for near in range(RING):
        out_ref[near * MESSAGE + LANES : (near + 1) * MESSAGE, :] = last


def merge(ring_ref, out_ref):
    low = lax.broadcasted_iota(jnp.int32, (1, LANES), 1) < HALF
    stats = [ring_ref[k * MESSAGE + LANES : (k + 1) * MESSAGE, :].astype(jnp.float32) for k in range(RING)]
    locals_, centers = [], []
    for stat in stats:
        one, two = stat[0:1], stat[1:2]
        turned = pltpu.roll(two, HALF, 1)
        locals_.append(one + pltpu.roll(one, HALF, 1) + jnp.where(low, two, turned))
        centers.append(jnp.where(low, turned, two))
    peak = functools.reduce(jnp.maximum, locals_)
    lse = peak + jnp.log(sum(jnp.exp(local - peak) for local in locals_))
    center = rounded(sum(centers) * (1.0 / RING))
    picked = jnp.zeros((LANES, LANES), jnp.float32)
    for k in range(RING):
        sent = ring_ref[k * MESSAGE : k * MESSAGE + LANES, :].astype(jnp.float32)
        picked = jnp.where(sent != 0.0, kept_off_zero(sent + (centers[k] - center)), picked)
    upper = rounded(lse)
    middle = rounded(lse - upper)
    lower = lse - upper - middle
    rows = out_ref.shape[0]
    row = lax.broadcasted_iota(jnp.int32, (rows, LANES), 0)
    lane = lax.broadcasted_iota(jnp.int32, (rows, LANES), 1)
    line = row % LINES
    order = ones_where((line < 2) & (lane == row // LINES * 2 + line))
    lines = jnp.dot(order, picked.astype(jnp.bfloat16), preferred_element_type=jnp.float32)
    lines = jnp.where(line == 2, jnp.where(low, upper, middle), lines)
    lines = jnp.where(line == 3, jnp.where(low, lower, center), lines)
    out_ref[...] = lines.astype(jnp.bfloat16)


def finish(all_ref, out_ref, lines_ref):
    lines_ref[...] = all_ref[...].astype(jnp.float32)
    sources = all_ref.shape[0] // LINES
    first = lines_ref[pl.ds(2, sources, stride=LINES), :]
    second = lines_ref[pl.ds(3, sources, stride=LINES), :]
    local = first + pltpu.roll(first, HALF, 1) + second
    low = lax.broadcasted_iota(jnp.int32, (1, LANES), 1) < HALF
    peak = jnp.max(local, axis=0, keepdims=True)
    mass = jnp.sum(jnp.exp(local - peak), axis=0, keepdims=True)
    lse = (peak + jnp.log(mass))[:, :HALF]
    center = jnp.where(low, pltpu.roll(second, HALF, 1), second)
    for pair in range(2):
        moved = lines_ref[pl.ds(pair, sources, stride=LINES), :]
        picked = jnp.sum(jnp.where(moved != 0.0, moved + center, 0.0), axis=0, keepdims=True)
        out_ref[2 * pair : 2 * pair + 1, :] = picked[:, :HALF] - lse
        out_ref[2 * pair + 1 : 2 * pair + 2, :] = picked[:, HALF:] - lse


VMEM = pl.BlockSpec(memory_space=pltpu.VMEM)


def on_chip(value):
    return pltpu.with_memory_space_constraint(value, pltpu.VMEM)


def exchanged(messages, groups):
    return lax.all_to_all(messages, CORPUS, split_axis=0, concat_axis=0, axis_index_groups=groups, tiled=True)


def body(queries, corpus, candidates):
    height, picks = candidates.shape
    size = lax.axis_size(CORPUS)
    first = first_rank([lax.axis_size(axis) for axis in CORPUS])
    both = lax.all_gather(corpus, "dim")
    sent = pl.pallas_call(
        functools.partial(pack, first),
        out_shape=pltpu.VMEM((RING * MESSAGE, LANES), jnp.bfloat16),
        in_specs=[VMEM, VMEM, VMEM],
        out_specs=VMEM,
        name="pack",
    )(on_chip(queries), on_chip(both), on_chip(candidates))
    planes = size // RING
    rings = [[plane * RING + (rank ^ (first % RING)) for rank in range(RING)] for plane in range(planes)]
    ring = exchanged(sent.reshape(RING, MESSAGE, LANES), rings)
    merged = pl.pallas_call(
        merge,
        out_shape=pltpu.VMEM((planes * LINES, LANES), jnp.bfloat16),
        in_specs=[VMEM],
        out_specs=VMEM,
        name="merge",
    )(on_chip(ring.reshape(RING * MESSAGE, LANES)))
    groups = [[(rank ^ (first // RING)) * RING + near for rank in range(planes)] for near in range(RING)]
    arrived = exchanged(merged.reshape(planes, LINES, LANES), groups)
    out = pl.pallas_call(
        finish,
        out_shape=jax.ShapeDtypeStruct((picks // size, height), jnp.float32),
        in_specs=[VMEM],
        out_specs=VMEM,
        scratch_shapes=[pltpu.VMEM((planes * LINES, LANES), jnp.float32)],
        name="finish",
    )(on_chip(arrived.reshape(planes * LINES, LANES)))
    return out.T


def solution(mesh):
    torus = Mesh(
        mesh.devices.reshape(8, 8, 4, mesh.shape["dim"]),
        (*CORPUS, "dim"),
    )
    return jax.shard_map(
        body,
        mesh=torus,
        in_specs=(P("dim", None), P(CORPUS, "dim"), P("dim", None)),
        out_specs=P("dim", CORPUS),
        check_vma=False,
    )
```

```python
import functools

import jax
import jax.numpy as jnp
from jax import lax
from jax.experimental import pallas as pl
from jax.experimental.pallas import tpu as pltpu
from jax.sharding import Mesh
from jax.sharding import PartitionSpec as P

CORPUS = ("corpus_0", "corpus_1", "corpus_2")
LANES = 128
HALF = LANES // 2
LINES = 4
RING = 4
TILE = 16
STATS = 8
MESSAGE = LANES + STATS
TINY = 1e-30
FIRST = (4, 4, 2)


def first_rank(shape):
    position = 0
    for at, size in zip(FIRST, shape):
        position = position * size + at
    return position


def lane_gather(table, lanes):
    numbers = lax.GatherDimensionNumbers(
        offset_dims=(),
        collapsed_slice_dims=(1,),
        start_index_map=(1,),
        operand_batching_dims=(0,),
        start_indices_batching_dims=(0,),
    )
    return lax.gather(
        table, lanes[:, :, None], numbers, slice_sizes=(1, 1), mode=lax.GatherScatterMode.PROMISE_IN_BOUNDS
    )


def matmul_nt(left, right):
    return lax.dot_general(left, right, (((1,), (1,)), ((), ())), preferred_element_type=jnp.float32)


def kept_off_zero(value):
    return jnp.where(jnp.abs(value) < TINY, TINY, value)


def rounded(value):
    return value.astype(jnp.bfloat16).astype(jnp.float32)


def ones_where(hit):
    return jnp.where(hit, 1.0, 0.0).astype(jnp.bfloat16)


def ring_order(first):
    row = lax.broadcasted_iota(jnp.int32, (HALF, LANES), 0)
    lane = lax.broadcasted_iota(jnp.int32, (HALF, LANES), 1)
    near = row // TILE ^ (first % RING)
    far = row % TILE // 2 ^ (first // RING % 8)
    slot = TILE * far + 4 * near + 2 * (row % 2)
    return jnp.concatenate([ones_where(lane == slot), ones_where(lane == slot + 1)], axis=1)


def pack(first, queries_ref, corpus_ref, candidates_ref, out_ref):
    width = corpus_ref.shape[2]
    scores = matmul_nt(queries_ref[:, :width], corpus_ref[0]) + matmul_nt(queries_ref[:, width:], corpus_ref[1])
    height, count = scores.shape
    order = ring_order(first)
    peak = jnp.max(scores, axis=1, keepdims=True)
    lse = peak + jnp.log(jnp.sum(jnp.exp(scores - peak), axis=1, keepdims=True))
    center = rounded(jnp.sum(scores, axis=1, keepdims=True) * (1.0 / count))
    moved = kept_off_zero(scores - center)
    upper = rounded(lse)
    middle = rounded(lse - upper)
    lower = lse - upper - middle
    low = lax.broadcasted_iota(jnp.int32, (height, LANES), 1) < HALF
    stats = jnp.concatenate([jnp.where(low, upper, lower), jnp.where(low, middle, center)], axis=0).astype(jnp.bfloat16)
    offset = lax.axis_index(CORPUS) * count
    nothing = jnp.zeros((height, LANES), jnp.bfloat16)
    for tile in range(candidates_ref.shape[1] // LANES):
        local = candidates_ref[:, tile * LANES : (tile + 1) * LANES] - offset
        block, lane = local >> 7, local & (LANES - 1)
        value = jnp.zeros((height, LANES), jnp.bfloat16)
        for w in range(count // LANES):
            got = lane_gather(moved[:, w * LANES : (w + 1) * LANES], lane).astype(jnp.bfloat16)
            value = jnp.where(block == w, got, value)
        both = jnp.concatenate(
            [jnp.concatenate([value, nothing], axis=0), jnp.concatenate([nothing, value], axis=0)], axis=1
        )
        lines = matmul_nt(order, both).astype(jnp.bfloat16)
        at = TILE * (tile ^ (first // RING // 8))
        for near in range(RING):
            out_ref[near * MESSAGE + at : near * MESSAGE + at + TILE, :] = lines[near * TILE : (near + 1) * TILE]
    row = lax.broadcasted_iota(jnp.int32, (STATS, LANES), 0)
    lane = lax.broadcasted_iota(jnp.int32, (STATS, LANES), 1)
    last = matmul_nt(ones_where((row < 2) & (lane == row * HALF)), stats).astype(jnp.bfloat16)
    for near in range(RING):
        out_ref[near * MESSAGE + LANES : (near + 1) * MESSAGE, :] = last


def merge(ring_ref, out_ref):
    low = lax.broadcasted_iota(jnp.int32, (1, LANES), 1) < HALF
    stats = [ring_ref[k * MESSAGE + LANES : (k + 1) * MESSAGE, :].astype(jnp.float32) for k in range(RING)]
    locals_, centers = [], []
    for stat in stats:
        one, two = stat[0:1], stat[1:2]
        turned = pltpu.roll(two, HALF, 1)
        locals_.append(one + pltpu.roll(one, HALF, 1) + jnp.where(low, two, turned))
        centers.append(jnp.where(low, turned, two))
    peak = functools.reduce(jnp.maximum, locals_)
    lse = peak + jnp.log(sum(jnp.exp(local - peak) for local in locals_))
    center = rounded(sum(centers) * (1.0 / RING))
    picked = jnp.zeros((LANES, LANES), jnp.float32)
    for k in range(RING):
        sent = ring_ref[k * MESSAGE : k * MESSAGE + LANES, :].astype(jnp.float32)
        picked = jnp.where(sent != 0.0, kept_off_zero(sent + (centers[k] - center)), picked)
    upper = rounded(lse)
    middle = rounded(lse - upper)
    lower = lse - upper - middle
    rows = out_ref.shape[0]
    row = lax.broadcasted_iota(jnp.int32, (rows, LANES), 0)
    lane = lax.broadcasted_iota(jnp.int32, (rows, LANES), 1)
    line = row % LINES
    order = ones_where((line < 2) & (lane == row // LINES * 2 + line))
    lines = jnp.dot(order, picked.astype(jnp.bfloat16), preferred_element_type=jnp.float32)
    lines = jnp.where(line == 2, jnp.where(low, upper, middle), lines)
    lines = jnp.where(line == 3, jnp.where(low, lower, center), lines)
    out_ref[...] = lines.astype(jnp.bfloat16)


def finish(all_ref, out_ref, lines_ref):
    lines_ref[...] = all_ref[...].astype(jnp.float32)
    sources = all_ref.shape[0] // LINES
    first = lines_ref[pl.ds(2, sources, stride=LINES), :]
    second = lines_ref[pl.ds(3, sources, stride=LINES), :]
    local = first + pltpu.roll(first, HALF, 1) + second
    low = lax.broadcasted_iota(jnp.int32, (1, LANES), 1) < HALF
    peak = jnp.max(local, axis=0, keepdims=True)
    mass = jnp.sum(jnp.exp(local - peak), axis=0, keepdims=True)
    lse = (peak + jnp.log(mass))[:, :HALF]
    center = jnp.where(low, pltpu.roll(second, HALF, 1), second)
    for pair in range(2):
        moved = lines_ref[pl.ds(pair, sources, stride=LINES), :]
        picked = jnp.sum(jnp.where(moved != 0.0, moved + center, 0.0), axis=0, keepdims=True)
        out_ref[2 * pair : 2 * pair + 1, :] = picked[:, :HALF] - lse
        out_ref[2 * pair + 1 : 2 * pair + 2, :] = picked[:, HALF:] - lse


VMEM = pl.BlockSpec(memory_space=pltpu.VMEM)


def on_chip(value):
    return pltpu.with_memory_space_constraint(value, pltpu.VMEM)


def exchanged(messages, groups):
    return lax.all_to_all(messages, CORPUS, split_axis=0, concat_axis=0, axis_index_groups=groups, tiled=True)


def body(queries, corpus, candidates):
    height, picks = candidates.shape
    size = lax.axis_size(CORPUS)
    first = first_rank([lax.axis_size(axis) for axis in CORPUS])
    both = lax.all_gather(corpus, "dim")
    sent = pl.pallas_call(
        functools.partial(pack, first),
        out_shape=pltpu.VMEM((RING * MESSAGE, LANES), jnp.bfloat16),
        in_specs=[VMEM, VMEM, VMEM],
        out_specs=VMEM,
        name="pack",
    )(on_chip(queries), on_chip(both), on_chip(candidates))
    planes = size // RING
    rings = [[plane * RING + (rank ^ (first % RING)) for rank in range(RING)] for plane in range(planes)]
    ring = exchanged(sent.reshape(RING, MESSAGE, LANES), rings)
    merged = pl.pallas_call(
        merge,
        out_shape=pltpu.VMEM((planes * LINES, LANES), jnp.bfloat16),
        in_specs=[VMEM],
        out_specs=VMEM,
        name="merge",
    )(on_chip(ring.reshape(RING * MESSAGE, LANES)))
    groups = [[(rank ^ (first // RING)) * RING + near for rank in range(planes)] for near in range(RING)]
    arrived = exchanged(merged.reshape(planes, LINES, LANES), groups)
    out = pl.pallas_call(
        finish,
        out_shape=jax.ShapeDtypeStruct((picks // size, height), jnp.float32),
        in_specs=[VMEM],
        out_specs=VMEM,
        scratch_shapes=[pltpu.VMEM((planes * LINES, LANES), jnp.float32)],
        name="finish",
    )(on_chip(arrived.reshape(planes * LINES, LANES)))
    return out.T


def solution(mesh):
    torus = Mesh(
        mesh.devices.reshape(8, 8, 4, mesh.shape["dim"]),
        (*CORPUS, "dim"),
    )
    return jax.shard_map(
        body,
        mesh=torus,
        in_specs=(P("dim", None), P(CORPUS, "dim"), P("dim", None)),
        out_specs=P("dim", CORPUS),
        check_vma=False,
    )
```

```python
import functools

import jax
import jax.numpy as jnp
from jax import lax
from jax.experimental import pallas as pl
from jax.experimental.pallas import tpu as pltpu
from jax.sharding import Mesh
from jax.sharding import PartitionSpec as P

CORPUS = ("corpus_0", "corpus_1", "corpus_2")
LANES = 128
HALF = LANES // 2
LINES = 4
RING = 4
TILE = 16
STATS = 8
MESSAGE = LANES + STATS
TINY = 1e-30
FIRST = (4, 4, 2)


def first_rank(shape):
    position = 0
    for at, size in zip(FIRST, shape):
        position = position * size + at
    return position


def lane_gather(table, lanes):
    numbers = lax.GatherDimensionNumbers(
        offset_dims=(),
        collapsed_slice_dims=(1,),
        start_index_map=(1,),
        operand_batching_dims=(0,),
        start_indices_batching_dims=(0,),
    )
    return lax.gather(
        table, lanes[:, :, None], numbers, slice_sizes=(1, 1), mode=lax.GatherScatterMode.PROMISE_IN_BOUNDS
    )


def matmul_nt(left, right):
    return lax.dot_general(left, right, (((1,), (1,)), ((), ())), preferred_element_type=jnp.float32)


def kept_off_zero(value):
    return jnp.where(jnp.abs(value) < TINY, TINY, value)


def rounded(value):
    return value.astype(jnp.bfloat16).astype(jnp.float32)


def ones_where(hit):
    return jnp.where(hit, 1.0, 0.0).astype(jnp.bfloat16)


def ring_order(first):
    row = lax.broadcasted_iota(jnp.int32, (HALF, LANES), 0)
    lane = lax.broadcasted_iota(jnp.int32, (HALF, LANES), 1)
    near = row // TILE ^ (first % RING)
    far = row % TILE // 2 ^ (first // RING % 8)
    slot = TILE * far + 4 * near + 2 * (row % 2)
    return jnp.concatenate([ones_where(lane == slot), ones_where(lane == slot + 1)], axis=1)


def pack(first, queries_ref, corpus_ref, candidates_ref, out_ref):
    _, count, width = corpus_ref.shape
    height = queries_ref.shape[0]
    part = count // 2
    scores = [
        matmul_nt(queries_ref[:, :width], corpus_ref[0, k * part : (k + 1) * part])
        + matmul_nt(queries_ref[:, width:], corpus_ref[1, k * part : (k + 1) * part])
        for k in range(2)
    ]
    center = rounded(jnp.sum(scores[0], axis=1, keepdims=True) * (1.0 / part))
    moved = [kept_off_zero(score - center) for score in scores]
    tables = [moved[w * LANES // part][:, w * LANES % part : w * LANES % part + LANES] for w in range(count // LANES)]
    order = ring_order(first)
    peak = jnp.max(jnp.maximum(scores[0], scores[1]), axis=1, keepdims=True)
    mass = jnp.sum(jnp.exp(scores[0] - peak) + jnp.exp(scores[1] - peak), axis=1, keepdims=True)
    lse = peak + jnp.log(mass)
    upper = rounded(lse)
    middle = rounded(lse - upper)
    lower = lse - upper - middle
    low = lax.broadcasted_iota(jnp.int32, (height, LANES), 1) < HALF
    stats = jnp.concatenate([jnp.where(low, upper, lower), jnp.where(low, middle, center)], axis=0).astype(jnp.bfloat16)
    offset = lax.axis_index(CORPUS) * count
    nothing = jnp.zeros((height, LANES), jnp.bfloat16)
    for tile in range(candidates_ref.shape[1] // LANES):
        local = candidates_ref[:, tile * LANES : (tile + 1) * LANES] - offset
        block, lane = local >> 7, local & (LANES - 1)
        value = jnp.zeros((height, LANES), jnp.bfloat16)
        for w in range(count // LANES):
            got = lane_gather(tables[w], lane).astype(jnp.bfloat16)
            value = jnp.where(block == w, got, value)
        both = jnp.concatenate(
            [jnp.concatenate([value, nothing], axis=0), jnp.concatenate([nothing, value], axis=0)], axis=1
        )
        lines = matmul_nt(order, both).astype(jnp.bfloat16)
        at = TILE * (tile ^ (first // RING // 8))
        for near in range(RING):
            out_ref[near * MESSAGE + at : near * MESSAGE + at + TILE, :] = lines[near * TILE : (near + 1) * TILE]
    row = lax.broadcasted_iota(jnp.int32, (STATS, LANES), 0)
    lane = lax.broadcasted_iota(jnp.int32, (STATS, LANES), 1)
    last = matmul_nt(ones_where((row < 2) & (lane == row * HALF)), stats).astype(jnp.bfloat16)
    for near in range(RING):
        out_ref[near * MESSAGE + LANES : (near + 1) * MESSAGE, :] = last


def merge(ring_ref, out_ref):
    low = lax.broadcasted_iota(jnp.int32, (1, LANES), 1) < HALF
    stats = [ring_ref[k * MESSAGE + LANES : (k + 1) * MESSAGE, :].astype(jnp.float32) for k in range(RING)]
    locals_, centers = [], []
    for stat in stats:
        one, two = stat[0:1], stat[1:2]
        turned = pltpu.roll(two, HALF, 1)
        locals_.append(one + pltpu.roll(one, HALF, 1) + jnp.where(low, two, turned))
        centers.append(jnp.where(low, turned, two))
    peak = functools.reduce(jnp.maximum, locals_)
    lse = peak + jnp.log(sum(jnp.exp(local - peak) for local in locals_))
    center = rounded(sum(centers) * (1.0 / RING))
    picked = jnp.zeros((LANES, LANES), jnp.float32)
    for k in range(RING):
        sent = ring_ref[k * MESSAGE : k * MESSAGE + LANES, :].astype(jnp.float32)
        picked = jnp.where(sent != 0.0, kept_off_zero(sent + (centers[k] - center)), picked)
    upper = rounded(lse)
    middle = rounded(lse - upper)
    lower = lse - upper - middle
    rows = out_ref.shape[0]
    row = lax.broadcasted_iota(jnp.int32, (rows, LANES), 0)
    lane = lax.broadcasted_iota(jnp.int32, (rows, LANES), 1)
    line = row % LINES
    order = ones_where((line < 2) & (lane == row // LINES * 2 + line))
    lines = jnp.dot(order, picked.astype(jnp.bfloat16), preferred_element_type=jnp.float32)
    lines = jnp.where(line == 2, jnp.where(low, upper, middle), lines)
    lines = jnp.where(line == 3, jnp.where(low, lower, center), lines)
    out_ref[...] = lines.astype(jnp.bfloat16)


def finish(all_ref, out_ref, lines_ref):
    lines_ref[...] = all_ref[...].astype(jnp.float32)
    sources = all_ref.shape[0] // LINES
    first = lines_ref[pl.ds(2, sources, stride=LINES), :]
    second = lines_ref[pl.ds(3, sources, stride=LINES), :]
    local = first + pltpu.roll(first, HALF, 1) + second
    low = lax.broadcasted_iota(jnp.int32, (1, LANES), 1) < HALF
    peak = jnp.max(local, axis=0, keepdims=True)
    mass = jnp.sum(jnp.exp(local - peak), axis=0, keepdims=True)
    lse = (peak + jnp.log(mass))[:, :HALF]
    center = jnp.where(low, pltpu.roll(second, HALF, 1), second)
    for pair in range(2):
        moved = lines_ref[pl.ds(pair, sources, stride=LINES), :]
        picked = jnp.sum(jnp.where(moved != 0.0, moved + center, 0.0), axis=0, keepdims=True)
        out_ref[2 * pair : 2 * pair + 1, :] = picked[:, :HALF] - lse
        out_ref[2 * pair + 1 : 2 * pair + 2, :] = picked[:, HALF:] - lse


VMEM = pl.BlockSpec(memory_space=pltpu.VMEM)


def on_chip(value):
    return pltpu.with_memory_space_constraint(value, pltpu.VMEM)


def exchanged(messages, groups):
    return lax.all_to_all(messages, CORPUS, split_axis=0, concat_axis=0, axis_index_groups=groups, tiled=True)


def body(queries, corpus, candidates):
    height, picks = candidates.shape
    size = lax.axis_size(CORPUS)
    first = first_rank([lax.axis_size(axis) for axis in CORPUS])
    both = lax.all_gather(corpus, "dim")
    sent = pl.pallas_call(
        functools.partial(pack, first),
        out_shape=pltpu.VMEM((RING * MESSAGE, LANES), jnp.bfloat16),
        in_specs=[VMEM, VMEM, VMEM],
        out_specs=VMEM,
        name="pack",
    )(on_chip(queries), on_chip(both), on_chip(candidates))
    planes = size // RING
    rings = [[plane * RING + (rank ^ (first % RING)) for rank in range(RING)] for plane in range(planes)]
    ring = exchanged(sent.reshape(RING, MESSAGE, LANES), rings)
    merged = pl.pallas_call(
        merge,
        out_shape=pltpu.VMEM((planes * LINES, LANES), jnp.bfloat16),
        in_specs=[VMEM],
        out_specs=VMEM,
        name="merge",
    )(on_chip(ring.reshape(RING * MESSAGE, LANES)))
    groups = [[(rank ^ (first // RING)) * RING + near for rank in range(planes)] for near in range(RING)]
    arrived = exchanged(merged.reshape(planes, LINES, LANES), groups)
    out = pl.pallas_call(
        finish,
        out_shape=jax.ShapeDtypeStruct((picks // size, height), jnp.float32),
        in_specs=[VMEM],
        out_specs=VMEM,
        scratch_shapes=[pltpu.VMEM((planes * LINES, LANES), jnp.float32)],
        name="finish",
    )(on_chip(arrived.reshape(planes * LINES, LANES)))
    return out.T


def solution(mesh):
    torus = Mesh(
        mesh.devices.reshape(8, 8, 4, mesh.shape["dim"]),
        (*CORPUS, "dim"),
    )
    return jax.shard_map(
        body,
        mesh=torus,
        in_specs=(P("dim", None), P(CORPUS, "dim"), P("dim", None)),
        out_specs=P("dim", CORPUS),
        check_vma=False,
    )
```

```python
import functools

import jax
import jax.numpy as jnp
from jax import lax
from jax.experimental import pallas as pl
from jax.experimental.pallas import tpu as pltpu
from jax.sharding import Mesh
from jax.sharding import PartitionSpec as P

CORPUS = ("corpus_0", "corpus_1", "corpus_2")
LANES = 128
HALF = LANES // 2
LINES = 4
RING = 4
TILE = 16
STATS = 8
MESSAGE = LANES + STATS
TINY = 1e-30
FIRST = (4, 4, 2)


def first_rank(shape):
    position = 0
    for at, size in zip(FIRST, shape):
        position = position * size + at
    return position


def lane_gather(table, lanes):
    numbers = lax.GatherDimensionNumbers(
        offset_dims=(),
        collapsed_slice_dims=(1,),
        start_index_map=(1,),
        operand_batching_dims=(0,),
        start_indices_batching_dims=(0,),
    )
    return lax.gather(
        table, lanes[:, :, None], numbers, slice_sizes=(1, 1), mode=lax.GatherScatterMode.PROMISE_IN_BOUNDS
    )


def matmul_nt(left, right):
    return lax.dot_general(left, right, (((1,), (1,)), ((), ())), preferred_element_type=jnp.float32)


def kept_off_zero(value):
    return jnp.where(jnp.abs(value) < TINY, TINY, value)


def rounded(value):
    return value.astype(jnp.bfloat16).astype(jnp.float32)


def ones_where(hit):
    return jnp.where(hit, 1.0, 0.0).astype(jnp.bfloat16)


def ring_order(first):
    row = lax.broadcasted_iota(jnp.int32, (HALF, LANES), 0)
    lane = lax.broadcasted_iota(jnp.int32, (HALF, LANES), 1)
    near = row // TILE ^ (first % RING)
    far = row % TILE // 2 ^ (first // RING % 8)
    slot = TILE * far + 4 * near + 2 * (row % 2)
    return jnp.concatenate([ones_where(lane == slot), ones_where(lane == slot + 1)], axis=1)


def pack(first, queries_ref, corpus_ref, candidates_ref, out_ref):
    _, count, width = corpus_ref.shape
    height = queries_ref.shape[0]
    part = count // 2
    scores = [
        matmul_nt(queries_ref[:, :width], corpus_ref[0, k * part : (k + 1) * part])
        + matmul_nt(queries_ref[:, width:], corpus_ref[1, k * part : (k + 1) * part])
        for k in range(2)
    ]
    center = rounded(jnp.sum(scores[0], axis=1, keepdims=True) * (1.0 / part))
    moved = [kept_off_zero(score - center) for score in scores]
    tables = [moved[w * LANES // part][:, w * LANES % part : w * LANES % part + LANES] for w in range(count // LANES)]
    order = ring_order(first)
    peak = jnp.max(jnp.maximum(scores[0], scores[1]), axis=1, keepdims=True)
    mass = jnp.sum(jnp.exp(scores[0] - peak) + jnp.exp(scores[1] - peak), axis=1, keepdims=True)
    lse = peak + jnp.log(mass)
    upper = rounded(lse)
    middle = rounded(lse - upper)
    lower = lse - upper - middle
    low = lax.broadcasted_iota(jnp.int32, (height, LANES), 1) < HALF
    stats = jnp.concatenate([jnp.where(low, upper, lower), jnp.where(low, middle, center)], axis=0).astype(jnp.bfloat16)
    offset = lax.axis_index(CORPUS) * count
    nothing = jnp.zeros((height, LANES), jnp.bfloat16)
    for tile in range(candidates_ref.shape[1] // LANES):
        values = []
        for top in range(0, height, 16):
            local = candidates_ref[top : top + 16, tile * LANES : (tile + 1) * LANES] - offset
            block, lane = local >> 7, local & (LANES - 1)
            value = jnp.zeros(local.shape, jnp.bfloat16)
            for w in range(count // LANES):
                got = lane_gather(tables[w][top : top + 16], lane).astype(jnp.bfloat16)
                value = jnp.where(block == w, got, value)
            values.append(value)
        value = jnp.concatenate(values, axis=0)
        both = jnp.concatenate(
            [jnp.concatenate([value, nothing], axis=0), jnp.concatenate([nothing, value], axis=0)], axis=1
        )
        lines = matmul_nt(order, both).astype(jnp.bfloat16)
        at = TILE * (tile ^ (first // RING // 8))
        for near in range(RING):
            out_ref[near * MESSAGE + at : near * MESSAGE + at + TILE, :] = lines[near * TILE : (near + 1) * TILE]
    row = lax.broadcasted_iota(jnp.int32, (STATS, LANES), 0)
    lane = lax.broadcasted_iota(jnp.int32, (STATS, LANES), 1)
    last = matmul_nt(ones_where((row < 2) & (lane == row * HALF)), stats).astype(jnp.bfloat16)
    for near in range(RING):
        out_ref[near * MESSAGE + LANES : (near + 1) * MESSAGE, :] = last


def merge(ring_ref, out_ref):
    low = lax.broadcasted_iota(jnp.int32, (1, LANES), 1) < HALF
    stats = [ring_ref[k * MESSAGE + LANES : (k + 1) * MESSAGE, :].astype(jnp.float32) for k in range(RING)]
    one = jnp.concatenate([stat[0:1] for stat in stats], axis=0)
    two = jnp.concatenate([stat[1:2] for stat in stats], axis=0)
    turned = pltpu.roll(two, HALF, 1)
    local = one + pltpu.roll(one, HALF, 1) + jnp.where(low, two, turned)
    peak = jnp.max(local, axis=0, keepdims=True)
    lse = peak + jnp.log(jnp.sum(jnp.exp(local - peak), axis=0, keepdims=True))
    centers = jnp.where(low, turned, two)
    center = rounded(jnp.sum(centers, axis=0, keepdims=True) * (1.0 / RING))
    picked = jnp.zeros((LANES, LANES), jnp.float32)
    for k in range(RING):
        sent = ring_ref[k * MESSAGE : k * MESSAGE + LANES, :].astype(jnp.float32)
        picked = jnp.where(sent != 0.0, kept_off_zero(sent + (centers[k : k + 1] - center)), picked)
    upper = rounded(lse)
    middle = rounded(lse - upper)
    lower = lse - upper - middle
    rows = out_ref.shape[0]
    row = lax.broadcasted_iota(jnp.int32, (rows, LANES), 0)
    lane = lax.broadcasted_iota(jnp.int32, (rows, LANES), 1)
    line = row % LINES
    order = ones_where((line < 2) & (lane == row // LINES * 2 + line))
    lines = jnp.dot(order, picked.astype(jnp.bfloat16), preferred_element_type=jnp.float32)
    lines = jnp.where(line == 2, jnp.where(low, upper, middle), lines)
    lines = jnp.where(line == 3, jnp.where(low, lower, center), lines)
    out_ref[...] = lines.astype(jnp.bfloat16)


def finish(all_ref, out_ref, lines_ref):
    lines_ref[...] = all_ref[...].astype(jnp.float32)
    sources = all_ref.shape[0] // LINES
    first = lines_ref[pl.ds(2, sources, stride=LINES), :]
    second = lines_ref[pl.ds(3, sources, stride=LINES), :]
    local = first + pltpu.roll(first, HALF, 1) + second
    low = lax.broadcasted_iota(jnp.int32, (1, LANES), 1) < HALF
    peak = jnp.max(local, axis=0, keepdims=True)
    mass = jnp.sum(jnp.exp(local - peak), axis=0, keepdims=True)
    lse = (peak + jnp.log(mass))[:, :HALF]
    center = jnp.where(low, pltpu.roll(second, HALF, 1), second)
    for pair in range(2):
        moved = lines_ref[pl.ds(pair, sources, stride=LINES), :]
        picked = jnp.sum(jnp.where(moved != 0.0, moved + center, 0.0), axis=0, keepdims=True)
        out_ref[2 * pair : 2 * pair + 1, :] = picked[:, :HALF] - lse
        out_ref[2 * pair + 1 : 2 * pair + 2, :] = picked[:, HALF:] - lse


VMEM = pl.BlockSpec(memory_space=pltpu.VMEM)


def on_chip(value):
    return pltpu.with_memory_space_constraint(value, pltpu.VMEM)


def exchanged(messages, groups):
    return lax.all_to_all(messages, CORPUS, split_axis=0, concat_axis=0, axis_index_groups=groups, tiled=True)


def body(queries, corpus, candidates):
    height, picks = candidates.shape
    size = lax.axis_size(CORPUS)
    first = first_rank([lax.axis_size(axis) for axis in CORPUS])
    both = lax.all_gather(corpus, "dim")
    sent = pl.pallas_call(
        functools.partial(pack, first),
        out_shape=pltpu.VMEM((RING * MESSAGE, LANES), jnp.bfloat16),
        in_specs=[VMEM, VMEM, VMEM],
        out_specs=VMEM,
        name="pack",
    )(on_chip(queries), on_chip(both), on_chip(candidates))
    planes = size // RING
    rings = [[plane * RING + (rank ^ (first % RING)) for rank in range(RING)] for plane in range(planes)]
    ring = exchanged(sent.reshape(RING, MESSAGE, LANES), rings)
    merged = pl.pallas_call(
        merge,
        out_shape=pltpu.VMEM((planes * LINES, LANES), jnp.bfloat16),
        in_specs=[VMEM],
        out_specs=VMEM,
        name="merge",
    )(on_chip(ring.reshape(RING * MESSAGE, LANES)))
    groups = [[(rank ^ (first // RING)) * RING + near for rank in range(planes)] for near in range(RING)]
    arrived = exchanged(merged.reshape(planes, LINES, LANES), groups)
    out = pl.pallas_call(
        finish,
        out_shape=jax.ShapeDtypeStruct((picks // size, height), jnp.float32),
        in_specs=[VMEM],
        out_specs=VMEM,
        scratch_shapes=[pltpu.VMEM((planes * LINES, LANES), jnp.float32)],
        name="finish",
    )(on_chip(arrived.reshape(planes * LINES, LANES)))
    return out.T


def solution(mesh):
    torus = Mesh(
        mesh.devices.reshape(8, 8, 4, mesh.shape["dim"]),
        (*CORPUS, "dim"),
    )
    return jax.shard_map(
        body,
        mesh=torus,
        in_specs=(P("dim", None), P(CORPUS, "dim"), P("dim", None)),
        out_specs=P("dim", CORPUS),
        check_vma=False,
    )
```

```python
import functools

import jax
import jax.numpy as jnp
from jax import lax
from jax.experimental import pallas as pl
from jax.experimental.pallas import tpu as pltpu
from jax.sharding import Mesh
from jax.sharding import PartitionSpec as P

CORPUS = ("corpus_0", "corpus_1", "corpus_2")
LANES = 128
HALF = LANES // 2
LINES = 4
RING = 4
TILE = 16
STATS = 8
MESSAGE = LANES + STATS
TINY = 1e-30
FIRST = (4, 5, 2)


def first_rank(shape):
    position = 0
    for at, size in zip(FIRST, shape):
        position = position * size + at
    return position


def lane_gather(table, lanes):
    numbers = lax.GatherDimensionNumbers(
        offset_dims=(),
        collapsed_slice_dims=(1,),
        start_index_map=(1,),
        operand_batching_dims=(0,),
        start_indices_batching_dims=(0,),
    )
    return lax.gather(
        table, lanes[:, :, None], numbers, slice_sizes=(1, 1), mode=lax.GatherScatterMode.PROMISE_IN_BOUNDS
    )


def matmul_nt(left, right):
    return lax.dot_general(left, right, (((1,), (1,)), ((), ())), preferred_element_type=jnp.float32)


def kept_off_zero(value):
    return jnp.where(jnp.abs(value) < TINY, TINY, value)


def rounded(value):
    return value.astype(jnp.bfloat16).astype(jnp.float32)


def ones_where(hit):
    return jnp.where(hit, 1.0, 0.0).astype(jnp.bfloat16)


def ring_order(first):
    row = lax.broadcasted_iota(jnp.int32, (HALF, LANES), 0)
    lane = lax.broadcasted_iota(jnp.int32, (HALF, LANES), 1)
    near = row // TILE ^ (first % RING)
    far = row % TILE // 2 ^ (first // RING % 8)
    slot = TILE * far + 4 * near + 2 * (row % 2)
    return jnp.concatenate([ones_where(lane == slot), ones_where(lane == slot + 1)], axis=1)


def pack(first, queries_ref, corpus_ref, candidates_ref, out_ref):
    _, count, width = corpus_ref.shape
    height = queries_ref.shape[0]
    part = count // 2
    scores = [
        matmul_nt(queries_ref[:, :width], corpus_ref[0, k * part : (k + 1) * part])
        + matmul_nt(queries_ref[:, width:], corpus_ref[1, k * part : (k + 1) * part])
        for k in range(2)
    ]
    center = rounded(jnp.sum(scores[0], axis=1, keepdims=True) * (1.0 / part))
    moved = [kept_off_zero(score - center) for score in scores]
    tables = [moved[w * LANES // part][:, w * LANES % part : w * LANES % part + LANES] for w in range(count // LANES)]
    order = ring_order(first)
    peak = jnp.max(jnp.maximum(scores[0], scores[1]), axis=1, keepdims=True)
    mass = jnp.sum(jnp.exp(scores[0] - peak) + jnp.exp(scores[1] - peak), axis=1, keepdims=True)
    lse = peak + jnp.log(mass)
    upper = rounded(lse)
    middle = rounded(lse - upper)
    lower = lse - upper - middle
    low = lax.broadcasted_iota(jnp.int32, (height, LANES), 1) < HALF
    stats = jnp.concatenate([jnp.where(low, upper, lower), jnp.where(low, middle, center)], axis=0).astype(jnp.bfloat16)
    offset = lax.axis_index(CORPUS) * count
    nothing = jnp.zeros((height, LANES), jnp.bfloat16)
    for tile in range(candidates_ref.shape[1] // LANES):
        values = []
        for top in range(0, height, 16):
            local = candidates_ref[top : top + 16, tile * LANES : (tile + 1) * LANES] - offset
            block, lane = local >> 7, local & (LANES - 1)
            value = jnp.zeros(local.shape, jnp.bfloat16)
            for w in range(count // LANES):
                got = lane_gather(tables[w][top : top + 16], lane).astype(jnp.bfloat16)
                value = jnp.where(block == w, got, value)
            values.append(value)
        value = jnp.concatenate(values, axis=0)
        both = jnp.concatenate(
            [jnp.concatenate([value, nothing], axis=0), jnp.concatenate([nothing, value], axis=0)], axis=1
        )
        lines = matmul_nt(order, both).astype(jnp.bfloat16)
        at = TILE * (tile ^ (first // RING // 8))
        for near in range(RING):
            out_ref[near * MESSAGE + at : near * MESSAGE + at + TILE, :] = lines[near * TILE : (near + 1) * TILE]
    row = lax.broadcasted_iota(jnp.int32, (STATS, LANES), 0)
    lane = lax.broadcasted_iota(jnp.int32, (STATS, LANES), 1)
    last = matmul_nt(ones_where((row < 2) & (lane == row * HALF)), stats).astype(jnp.bfloat16)
    for near in range(RING):
        out_ref[near * MESSAGE + LANES : (near + 1) * MESSAGE, :] = last


def merge(ring_ref, out_ref):
    low = lax.broadcasted_iota(jnp.int32, (1, LANES), 1) < HALF
    stats = [ring_ref[k * MESSAGE + LANES : (k + 1) * MESSAGE, :].astype(jnp.float32) for k in range(RING)]
    one = jnp.concatenate([stat[0:1] for stat in stats], axis=0)
    two = jnp.concatenate([stat[1:2] for stat in stats], axis=0)
    turned = pltpu.roll(two, HALF, 1)
    local = one + pltpu.roll(one, HALF, 1) + jnp.where(low, two, turned)
    peak = jnp.max(local, axis=0, keepdims=True)
    lse = peak + jnp.log(jnp.sum(jnp.exp(local - peak), axis=0, keepdims=True))
    centers = jnp.where(low, turned, two)
    center = rounded(jnp.sum(centers, axis=0, keepdims=True) * (1.0 / RING))
    picked = jnp.zeros((LANES, LANES), jnp.float32)
    for k in range(RING):
        sent = ring_ref[k * MESSAGE : k * MESSAGE + LANES, :].astype(jnp.float32)
        picked = jnp.where(sent != 0.0, kept_off_zero(sent + (centers[k : k + 1] - center)), picked)
    upper = rounded(lse)
    middle = rounded(lse - upper)
    lower = lse - upper - middle
    rows = out_ref.shape[0]
    row = lax.broadcasted_iota(jnp.int32, (rows, LANES), 0)
    lane = lax.broadcasted_iota(jnp.int32, (rows, LANES), 1)
    line = row % LINES
    order = ones_where((line < 2) & (lane == row // LINES * 2 + line))
    lines = jnp.dot(order, picked.astype(jnp.bfloat16), preferred_element_type=jnp.float32)
    lines = jnp.where(line == 2, jnp.where(low, upper, middle), lines)
    lines = jnp.where(line == 3, jnp.where(low, lower, center), lines)
    out_ref[...] = lines.astype(jnp.bfloat16)


def finish(all_ref, out_ref, lines_ref):
    lines_ref[...] = all_ref[...].astype(jnp.float32)
    sources = all_ref.shape[0] // LINES
    first = lines_ref[pl.ds(2, sources, stride=LINES), :]
    second = lines_ref[pl.ds(3, sources, stride=LINES), :]
    local = first + pltpu.roll(first, HALF, 1) + second
    low = lax.broadcasted_iota(jnp.int32, (1, LANES), 1) < HALF
    peak = jnp.max(local, axis=0, keepdims=True)
    mass = jnp.sum(jnp.exp(local - peak), axis=0, keepdims=True)
    lse = (peak + jnp.log(mass))[:, :HALF]
    center = jnp.where(low, pltpu.roll(second, HALF, 1), second)
    for pair in range(2):
        moved = lines_ref[pl.ds(pair, sources, stride=LINES), :]
        picked = jnp.sum(jnp.where(moved != 0.0, moved + center, 0.0), axis=0, keepdims=True)
        out_ref[2 * pair : 2 * pair + 1, :] = picked[:, :HALF] - lse
        out_ref[2 * pair + 1 : 2 * pair + 2, :] = picked[:, HALF:] - lse


VMEM = pl.BlockSpec(memory_space=pltpu.VMEM)


def on_chip(value):
    return pltpu.with_memory_space_constraint(value, pltpu.VMEM)


def exchanged(messages, groups):
    return lax.all_to_all(messages, CORPUS, split_axis=0, concat_axis=0, axis_index_groups=groups, tiled=True)


def body(queries, corpus, candidates):
    height, picks = candidates.shape
    size = lax.axis_size(CORPUS)
    first = first_rank([lax.axis_size(axis) for axis in CORPUS])
    both = lax.all_gather(corpus, "dim")
    sent = pl.pallas_call(
        functools.partial(pack, first),
        out_shape=pltpu.VMEM((RING * MESSAGE, LANES), jnp.bfloat16),
        in_specs=[VMEM, VMEM, VMEM],
        out_specs=VMEM,
        name="pack",
    )(on_chip(queries), on_chip(both), on_chip(candidates))
    planes = size // RING
    rings = [[plane * RING + (rank ^ (first % RING)) for rank in range(RING)] for plane in range(planes)]
    ring = exchanged(sent.reshape(RING, MESSAGE, LANES), rings)
    merged = pl.pallas_call(
        merge,
        out_shape=pltpu.VMEM((planes * LINES, LANES), jnp.bfloat16),
        in_specs=[VMEM],
        out_specs=VMEM,
        name="merge",
    )(on_chip(ring.reshape(RING * MESSAGE, LANES)))
    groups = [[(rank ^ (first // RING)) * RING + near for rank in range(planes)] for near in range(RING)]
    arrived = exchanged(merged.reshape(planes, LINES, LANES), groups)
    out = pl.pallas_call(
        finish,
        out_shape=jax.ShapeDtypeStruct((picks // size, height), jnp.float32),
        in_specs=[VMEM],
        out_specs=VMEM,
        scratch_shapes=[pltpu.VMEM((planes * LINES, LANES), jnp.float32)],
        name="finish",
    )(on_chip(arrived.reshape(planes * LINES, LANES)))
    return out.T


def solution(mesh):
    torus = Mesh(
        mesh.devices.reshape(8, 8, 4, mesh.shape["dim"]),
        (*CORPUS, "dim"),
    )
    return jax.shard_map(
        body,
        mesh=torus,
        in_specs=(P("dim", None), P(CORPUS, "dim"), P("dim", None)),
        out_specs=P("dim", CORPUS),
        check_vma=False,
    )
```

```python
import functools

import jax
import jax.numpy as jnp
from jax import lax
from jax.experimental import pallas as pl
from jax.experimental.pallas import tpu as pltpu
from jax.sharding import Mesh
from jax.sharding import PartitionSpec as P

CORPUS = ("corpus_0", "corpus_1", "corpus_2")
LANES = 128
HALF = LANES // 2
LINES = 4
RING = 4
TILE = 16
STATS = 8
MESSAGE = LANES + STATS
TINY = 1e-30
FIRST = (4, 5, 2)


def first_rank(shape):
    position = 0
    for at, size in zip(FIRST, shape):
        position = position * size + at
    return position


def lane_gather(table, lanes):
    numbers = lax.GatherDimensionNumbers(
        offset_dims=(),
        collapsed_slice_dims=(1,),
        start_index_map=(1,),
        operand_batching_dims=(0,),
        start_indices_batching_dims=(0,),
    )
    return lax.gather(
        table, lanes[:, :, None], numbers, slice_sizes=(1, 1), mode=lax.GatherScatterMode.PROMISE_IN_BOUNDS
    )


def matmul_nt(left, right):
    return lax.dot_general(left, right, (((1,), (1,)), ((), ())), preferred_element_type=jnp.float32)


def kept_off_zero(value):
    return jnp.where(jnp.abs(value) < TINY, TINY, value)


def rounded(value):
    return value.astype(jnp.bfloat16).astype(jnp.float32)


def ones_where(hit):
    return jnp.where(hit, 1.0, 0.0).astype(jnp.bfloat16)


def ring_order(first):
    row = lax.broadcasted_iota(jnp.int32, (HALF, LANES), 0)
    lane = lax.broadcasted_iota(jnp.int32, (HALF, LANES), 1)
    near = row // TILE ^ (first % RING)
    far = row % TILE // 2 ^ (first // RING % 8)
    slot = TILE * far + 4 * near + 2 * (row % 2)
    return jnp.concatenate([ones_where(lane == slot), ones_where(lane == slot + 1)], axis=1)


def pack(first, queries_ref, corpus_ref, candidates_ref, out_ref):
    _, count, width = corpus_ref.shape
    height = queries_ref.shape[0]
    part = count // 2
    scores = [
        matmul_nt(queries_ref[:, :width], corpus_ref[1, k * part : (k + 1) * part])
        + matmul_nt(queries_ref[:, width:], corpus_ref[0, k * part : (k + 1) * part])
        for k in range(2)
    ]
    center = rounded(jnp.sum(scores[0], axis=1, keepdims=True) * (1.0 / part))
    moved = [kept_off_zero(score - center) for score in scores]
    tables = [moved[w * LANES // part][:, w * LANES % part : w * LANES % part + LANES] for w in range(count // LANES)]
    order = ring_order(first)
    peak = jnp.max(jnp.maximum(scores[0], scores[1]), axis=1, keepdims=True)
    mass = jnp.sum(jnp.exp(scores[0] - peak) + jnp.exp(scores[1] - peak), axis=1, keepdims=True)
    lse = peak + jnp.log(mass)
    upper = rounded(lse)
    middle = rounded(lse - upper)
    lower = lse - upper - middle
    low = lax.broadcasted_iota(jnp.int32, (height, LANES), 1) < HALF
    stats = jnp.concatenate([jnp.where(low, upper, lower), jnp.where(low, middle, center)], axis=0).astype(jnp.bfloat16)
    offset = lax.axis_index(CORPUS) * count
    nothing = jnp.zeros((height, LANES), jnp.bfloat16)
    for tile in range(candidates_ref.shape[1] // LANES):
        values = []
        for top in range(0, height, 16):
            local = candidates_ref[top : top + 16, tile * LANES : (tile + 1) * LANES] - offset
            block, lane = local >> 7, local & (LANES - 1)
            value = jnp.zeros(local.shape, jnp.bfloat16)
            for w in range(count // LANES):
                got = lane_gather(tables[w][top : top + 16], lane).astype(jnp.bfloat16)
                value = jnp.where(block == w, got, value)
            values.append(value)
        value = jnp.concatenate(values, axis=0)
        both = jnp.concatenate(
            [jnp.concatenate([value, nothing], axis=0), jnp.concatenate([nothing, value], axis=0)], axis=1
        )
        lines = matmul_nt(order, both).astype(jnp.bfloat16)
        at = TILE * (tile ^ (first // RING // 8))
        for near in range(RING):
            out_ref[near * MESSAGE + at : near * MESSAGE + at + TILE, :] = lines[near * TILE : (near + 1) * TILE]
    row = lax.broadcasted_iota(jnp.int32, (STATS, LANES), 0)
    lane = lax.broadcasted_iota(jnp.int32, (STATS, LANES), 1)
    last = matmul_nt(ones_where((row < 2) & (lane == row * HALF)), stats).astype(jnp.bfloat16)
    for near in range(RING):
        out_ref[near * MESSAGE + LANES : (near + 1) * MESSAGE, :] = last


def merge(ring_ref, out_ref):
    low = lax.broadcasted_iota(jnp.int32, (1, LANES), 1) < HALF
    stats = [ring_ref[k * MESSAGE + LANES : (k + 1) * MESSAGE, :].astype(jnp.float32) for k in range(RING)]
    one = jnp.concatenate([stat[0:1] for stat in stats], axis=0)
    two = jnp.concatenate([stat[1:2] for stat in stats], axis=0)
    turned = pltpu.roll(two, HALF, 1)
    local = one + pltpu.roll(one, HALF, 1) + jnp.where(low, two, turned)
    peak = jnp.max(local, axis=0, keepdims=True)
    lse = peak + jnp.log(jnp.sum(jnp.exp(local - peak), axis=0, keepdims=True))
    centers = jnp.where(low, turned, two)
    center = rounded(jnp.sum(centers, axis=0, keepdims=True) * (1.0 / RING))
    picked = jnp.zeros((LANES, LANES), jnp.float32)
    for k in range(RING):
        sent = ring_ref[k * MESSAGE : k * MESSAGE + LANES, :].astype(jnp.float32)
        picked = jnp.where(sent != 0.0, kept_off_zero(sent + (centers[k : k + 1] - center)), picked)
    upper = rounded(lse)
    middle = rounded(lse - upper)
    lower = lse - upper - middle
    rows = out_ref.shape[0]
    row = lax.broadcasted_iota(jnp.int32, (rows, LANES), 0)
    lane = lax.broadcasted_iota(jnp.int32, (rows, LANES), 1)
    line = row % LINES
    order = ones_where((line < 2) & (lane == row // LINES * 2 + line))
    lines = jnp.dot(order, picked.astype(jnp.bfloat16), preferred_element_type=jnp.float32)
    lines = jnp.where(line == 2, jnp.where(low, upper, middle), lines)
    lines = jnp.where(line == 3, jnp.where(low, lower, center), lines)
    out_ref[...] = lines.astype(jnp.bfloat16)


def finish(all_ref, out_ref, lines_ref):
    lines_ref[...] = all_ref[...].astype(jnp.float32)
    sources = all_ref.shape[0] // LINES
    first = lines_ref[pl.ds(2, sources, stride=LINES), :]
    second = lines_ref[pl.ds(3, sources, stride=LINES), :]
    local = first + pltpu.roll(first, HALF, 1) + second
    low = lax.broadcasted_iota(jnp.int32, (1, LANES), 1) < HALF
    peak = jnp.max(local, axis=0, keepdims=True)
    mass = jnp.sum(jnp.exp(local - peak), axis=0, keepdims=True)
    lse = (peak + jnp.log(mass))[:, :HALF]
    center = jnp.where(low, pltpu.roll(second, HALF, 1), second)
    for pair in range(2):
        moved = lines_ref[pl.ds(pair, sources, stride=LINES), :]
        picked = jnp.sum(jnp.where(moved != 0.0, moved + center, 0.0), axis=0, keepdims=True)
        out_ref[2 * pair : 2 * pair + 1, :] = picked[:, :HALF] - lse
        out_ref[2 * pair + 1 : 2 * pair + 2, :] = picked[:, HALF:] - lse


VMEM = pl.BlockSpec(memory_space=pltpu.VMEM)


def on_chip(value):
    return pltpu.with_memory_space_constraint(value, pltpu.VMEM)


def exchanged(messages, groups):
    return lax.all_to_all(messages, CORPUS, split_axis=0, concat_axis=0, axis_index_groups=groups, tiled=True)


def body(queries, corpus, candidates):
    height, picks = candidates.shape
    size = lax.axis_size(CORPUS)
    first = first_rank([lax.axis_size(axis) for axis in CORPUS])
    both = lax.all_gather(corpus, "dim", axis_index_groups=[[1, 0]])
    sent = pl.pallas_call(
        functools.partial(pack, first),
        out_shape=pltpu.VMEM((RING * MESSAGE, LANES), jnp.bfloat16),
        in_specs=[VMEM, VMEM, VMEM],
        out_specs=VMEM,
        name="pack",
    )(on_chip(queries), on_chip(both), on_chip(candidates))
    planes = size // RING
    rings = [[plane * RING + (rank ^ (first % RING)) for rank in range(RING)] for plane in range(planes)]
    ring = exchanged(sent.reshape(RING, MESSAGE, LANES), rings)
    merged = pl.pallas_call(
        merge,
        out_shape=pltpu.VMEM((planes * LINES, LANES), jnp.bfloat16),
        in_specs=[VMEM],
        out_specs=VMEM,
        name="merge",
    )(on_chip(ring.reshape(RING * MESSAGE, LANES)))
    groups = [[(rank ^ (first // RING)) * RING + near for rank in range(planes)] for near in range(RING)]
    arrived = exchanged(merged.reshape(planes, LINES, LANES), groups)
    out = pl.pallas_call(
        finish,
        out_shape=jax.ShapeDtypeStruct((picks // size, height), jnp.float32),
        in_specs=[VMEM],
        out_specs=VMEM,
        scratch_shapes=[pltpu.VMEM((planes * LINES, LANES), jnp.float32)],
        name="finish",
    )(on_chip(arrived.reshape(planes * LINES, LANES)))
    return out.T


def solution(mesh):
    torus = Mesh(
        mesh.devices.reshape(8, 8, 4, mesh.shape["dim"]),
        (*CORPUS, "dim"),
    )
    return jax.shard_map(
        body,
        mesh=torus,
        in_specs=(P("dim", None), P(CORPUS, "dim"), P("dim", None)),
        out_specs=P("dim", CORPUS),
        check_vma=False,
    )
```
